32 devices in a mesh: grp: 8 (over y, x, core), sub: 4 (over z).
Axes of the slice: x: 2, y: 2, z: 4, core: 2. Of those that a mesh axis runs over, the one named last changes fastest.
Arguments:
- master: float32 [4096, 3584], P(('grp', 'sub')), may hold values from -120 to 120
- moment_one: float32 [4096, 3584], P(('grp', 'sub')), may hold values from -6 to 6
- moment_two: float32 [4096, 3584], P(('grp', 'sub')), may hold values from 0.01 to 4
- gradient: float32 [4096, 3584], P(('grp', 'sub')), may hold values from -120 to 120
- partner: int32 [32], replicated, may hold values from 0 to 31, each once
- tensor_of_row: int32 [4096], replicated, may hold values from 0 to 7, never falling along the last dimension, each value on 1 to 1024 neighbouring positions
Outputs:
- new_master: float32 [4096, 3584], P(('grp', 'sub'))
- new_moment_one: float32 [4096, 3584], P(('grp', 'sub'))
- new_moment_two: float32 [4096, 3584], P(('grp', 'sub'))
The draws below stay inside these ranges and needn't reach their ends.
Inputs may be any that keep to these rules, and one draw needn't show every extreme that they name: partner[n] is the device of new rank n; every device holds exactly one rank. `tensor_of_row`: tensor numbers never fall along the rows; each of the 8 tensors has one or more rows.
All inputs are finite; a program needn't handle non-finite values.
Results may differ from the reference program's by a relative error of at most 0.00007.
Values sent between devices are 32-bit elements; how exact they have to be, the bound alone decides.
A program may use at most 128 MiB of HBM per device.

```python
import math
import jax
import jax.numpy as jnp
import numpy as np
from jax import lax

W = 3584
ROWS_DEV = 128
LAYERS = 8
NDEV = 32
ROWS = 4096
BLOCK = 4


def scale_field(key, trend_pos):
    key_row, key_col = jax.random.split(key, 2)
    row_scale = jnp.exp(jax.random.uniform(key_row, (ROWS, 1), jnp.float32, 0.0, math.log(10.0)))
    col_scale = jnp.exp(jax.random.uniform(key_col, (1, W), jnp.float32, 0.0, math.log(10.0)))
    trend = jnp.power(3.0, trend_pos.astype(jnp.float32) / max(NDEV - 1, 1))
    return row_scale * col_scale * trend[:, None] / 15.0


def draw_master(key, part):
    key = jax.random.fold_in(key, 11)
    key_scale, key_noise = jax.random.split(key, 2)
    row_index = jnp.arange(ROWS, dtype=jnp.int32)
    trend_pos = row_index % ROWS_DEV // BLOCK
    noise = jax.random.normal(key_noise, (ROWS, W), jnp.float32)
    noise = jnp.clip(noise, -6.0, 6.0)
    return noise * scale_field(key_scale, trend_pos)


def draw_gradient(key, part):
    key = jax.random.fold_in(key, 23)
    key_scale, key_noise = jax.random.split(key, 2)
    row_index = jnp.arange(ROWS, dtype=jnp.int32)
    trend_pos = row_index // ROWS_DEV
    noise = jax.random.normal(key_noise, (ROWS, W), jnp.float32)
    noise = jnp.clip(noise, -6.0, 6.0)
    return noise * scale_field(key_scale, trend_pos)


def steps_of(rng, dims, pieces, smallest, top_value):
    gain, own = 1.0, jax.random.fold_in(rng, 6)
    for dim, shards_of in pieces:
        steps = jnp.exp(jax.random.uniform(jax.random.fold_in(own, dim), (shards_of,), jnp.float32, smallest / len(pieces), top_value / len(pieces)))
        gain = gain * jnp.repeat(steps, dims[dim] // shards_of).reshape([-1 if axis == dim else 1 for axis in range(len(dims))])
    return gain


def profile(count, total, bound, slope):
    loads = [(1 << 20) // math.isqrt(standing ** slope) + 1 for standing in range(2, count + 1)]
    surplus, given = total - bound - (count - 1), [1] * (count - 1)
    while surplus > 0:
        candidates = [i for i in range(count - 1) if given[i] < bound]
        pool, remaining = sum([loads[i] for i in candidates]), surplus
        for i in candidates:
            extra = min(bound - given[i], max(1, remaining * loads[i] // pool), surplus)
            given[i] = given[i] + extra
            surplus = surplus - extra
    return np.array([bound] + given)


def ragged_sizes(rng, number_of, total, bound, slope):
    if number_of == 2:
        one = jax.random.randint(rng, (), max(1, total - bound), min(bound, total - 1) + 1)
        return jnp.stack([one, total - one])
    sizes = jnp.asarray(profile(number_of, total, bound, slope), jnp.int32)
    twos = (number_of - 1) // 2
    donor, sink = sizes[1:1 + 2 * twos:2], sizes[2:2 + 2 * twos:2]
    slack = jnp.minimum(donor - 1, bound - sink)
    shifted = jax.random.randint(jax.random.fold_in(rng, 1), (twos,), 0, 1 << 20) % (slack + 1)
    sizes = sizes.at[1:1 + 2 * twos:2].set(donor - shifted).at[2:2 + 2 * twos:2].set(sink + shifted)
    return sizes[jax.random.permutation(jax.random.fold_in(rng, 2), number_of)]


def gaussian(own_key, extent, spread, bound, cuts=(), kind=jnp.bfloat16):
    entries = jax.random.normal(own_key, extent, jnp.float32) * spread
    if len(cuts) > 0:
        entries = steps_of(own_key, extent, cuts, -0.22, 0.18) * entries
    return jnp.clip(entries, min=-bound, max=bound).astype(kind)


def setup_inputs(seed: int = 0) -> dict:
    keys = jax.random.split(jax.random.key(seed), 7)
    return {
        "master": draw_master(jax.random.fold_in(keys[6], 71), 0),
        "moment_one": gaussian(keys[1], (ROWS, W), 1.0, 6.0, ((0, 32),), jnp.float32),
        "moment_two": jnp.clip(jnp.exp(math.log(4.0) - 5.9914646 * jax.random.uniform(keys[2], (ROWS, W), jnp.float32) ** steps_of(keys[2], (ROWS, W), ((0, 32),), -0.2, 0.2)), 0.01, 4.0),
        "gradient": draw_gradient(jax.random.fold_in(keys[6], 71), 0),
        "partner": jax.random.permutation(keys[4], NDEV).astype(jnp.int32),
        "tensor_of_row": jnp.searchsorted(jnp.cumsum(ragged_sizes(keys[5], LAYERS, ROWS, 2 * ROWS // LAYERS, 1)), jnp.arange(ROWS), side="right").astype(jnp.int32),
    }


beta_one = 0.9
beta_two = 0.999
step_count = 10
adam_eps = 1e-06
trust_eps = 1e-06
learn_rate = 0.05
decay_rate = 0.01

def reference(master, moment_one, moment_two, gradient, partner, tensor_of_row):
    total_rows = master.shape[0]
    row_index = jnp.arange(total_rows, dtype=jnp.int32)
    owner = row_index // ROWS_DEV
    inside = row_index % ROWS_DEV
    rank = inside // BLOCK
    offset = inside % BLOCK
    place = (partner[rank] * ROWS_DEV + owner * BLOCK + offset).astype(jnp.int32)
    grad_rows = gradient[place]
    first = beta_one * moment_one + (1.0 - beta_one) * grad_rows
    second = beta_two * moment_two + (1.0 - beta_two) * grad_rows * grad_rows
    correct_one = 1.0 - beta_one ** step_count
    correct_two = 1.0 - beta_two ** step_count
    update = first / correct_one / (jnp.sqrt(second / correct_two) + adam_eps) + decay_rate * master
    weight_sq = jax.ops.segment_sum(lax.optimization_barrier(jnp.sum(master * master, axis=1)), tensor_of_row, num_segments=LAYERS)
    update_sq = jax.ops.segment_sum(lax.optimization_barrier(jnp.sum(update * update, axis=1)), tensor_of_row, num_segments=LAYERS)
    ratio = jnp.sqrt(weight_sq) / (jnp.sqrt(update_sq) + trust_eps)
    row_ratio = ratio[tensor_of_row]
    fresh = master - learn_rate * row_ratio[:, None] * update

    def settle(values):
        return jnp.zeros_like(values).at[place].set(values)
    return (settle(fresh), settle(first), settle(second))
```

```python
import functools

import jax
import jax.numpy as jnp
from jax import lax
from jax.experimental import pallas as pl
from jax.experimental.pallas import tpu as pltpu
from jax.sharding import PartitionSpec as P

LAYERS = 8
LANES = 128
TILE = 8
PIECES = 4
MESH = pl.DeviceIdType.MESH

beta_one = 0.9
beta_two = 0.999
step_count = 10
adam_eps = 1e-06
trust_eps = 1e-06
learn_rate = 0.05
decay_rate = 0.01


def xor(a, b, bound):
    total, bit = 0, 1
    while bit < bound:
        total = total + ((a // bit + b // bit) % 2) * bit
        bit *= 2
    return total


def flips(here, bound):
    steps, bit = [], 1
    while bit < bound:
        steps.append(bit - 2 * bit * ((here // bit) % 2))
        bit *= 2
    return [
        here + sum(step for b, step in enumerate(steps) if (k >> b) % 2) for k in range(bound)
    ]


def sub_order(subs):
    width = subs.bit_length() - 1
    codes = [i ^ (i >> 1) for i in range(subs)]
    return [sum(((c >> b) & 1) << (width - 1 - b) for b in range(width)) for c in codes]


def kernel(groups, subs, partner_hbm, ids_hbm, master_hbm, one_hbm, two_hbm, grad_hbm,
           weights, update, first_out, second_out, row_ids, ratio_out,
           partner, ids, master, one, two, grad, staged, landed, acc_w, acc_u, sums,
           load_sem, send_sem, recv_sem, sum_send, sum_recv):
    devices = groups * subs
    rows_dev, width = grad.shape
    block = rows_dev // devices
    many = TILE // block
    columns = width // LANES
    my_grp, my_sub = lax.axis_index("grp"), lax.axis_index("sub")
    me = my_grp * subs + my_sub
    grps, sbs = flips(my_grp, groups), flips(my_sub, subs)
    order = sub_order(subs)
    send_order = order[1:] + order[:1]
    take_order = [s for s in order if s != subs - 1] + [subs - 1]
    peers = [g * subs + s for s in send_order for g in range(groups) if g or s]

    loads = [
        pltpu.make_async_copy(src, dst, load_sem.at[i])
        for i, (src, dst) in enumerate([
            (partner_hbm, partner), (master_hbm, master), (one_hbm, one), (two_hbm, two),
            (ids_hbm, ids), (grad_hbm, grad),
        ])
    ]
    for load in loads:
        load.start()

    def at(k):
        return {"grp": grps[k // subs], "sub": sbs[k % subs]}

    barrier = pltpu.get_barrier_semaphore()
    for k in reversed(peers):
        pl.semaphore_signal(barrier, inc=1, device_id=at(k), device_id_type=MESH)

    def across(g, s):
        return {"grp": xor(my_grp, g, groups), "sub": xor(my_sub, s, subs)}

    def exchange(g, s):
        there, k = across(g, s), g * subs + s
        return pltpu.make_async_remote_copy(
            src_ref=staged.at[k],
            dst_ref=landed.at[k],
            send_sem=send_sem.at[k],
            recv_sem=recv_sem.at[k],
            device_id=there,
            device_id_type=MESH,
        )

    def exchange_sum(k):
        return pltpu.make_async_remote_copy(
            src_ref=sums.at[0],
            dst_ref=sums.at[k],
            send_sem=sum_send.at[k],
            recv_sem=sum_recv.at[k],
            device_id=at(k),
            device_id_type=MESH,
        )

    def rank_of(device):
        def seek(n, found):
            return jnp.where(partner[n] == device, n, found)

        return lax.fori_loop(0, devices, seek, jnp.int32(0), unroll=8)

    def tile_of(place):
        return pl.ds(pl.multiple_of(place // many * TILE, TILE), TILE)

    loads[0].wait()

    def stage(g, s, target):
        there = across(g, s)
        rank = rank_of(there["grp"] * subs + there["sub"])
        slab, part = rank // many, jnp.full((block, LANES), rank % many, jnp.int32)
        for a, source in enumerate((master, one, two)):
            for c in range(columns):
                cut = slice(c * LANES, (c + 1) * LANES)
                tile = source[slab, :, cut]
                piece = tile[:block]
                for i in range(1, many):
                    piece = jnp.where(part == i, tile[i * block : (i + 1) * block], piece)
                target[a, :, cut] = piece

    for load in loads[1:4]:
        load.wait()
    for s in send_order:
        last = 0 if s else 1
        stage(groups - 1, s, staged.at[(groups - 1) * subs + s])
        if s == send_order[0]:
            pl.semaphore_wait(barrier, devices - 1)

        def send(i, carry, s=s):
            g = groups - 1 - i
            stage(g - 1, s, staged.at[(g - 1) * subs + s])
            exchange(g, s).start()
            return carry

        lax.fori_loop(0, groups - 1 - last, send, 0)
        exchange(last, s).start()
    stage(0, 0, landed.at[0])
    my_rank = rank_of(me)
    loads[4].wait()
    loads[5].wait()
    acc_w[...] = jnp.zeros_like(acc_w)
    acc_u[...] = jnp.zeros_like(acc_u)
    sub_iota = lax.broadcasted_iota(jnp.int32, (TILE, LANES), 0)
    lane_iota = lax.broadcasted_iota(jnp.int32, (TILE, LANES), 1)
    scale_one = 1.0 / (1.0 - beta_one**step_count)
    scale_two = 1.0 / (1.0 - beta_two**step_count)

    def consume(g, s):
        there, k = across(g, s), g * subs + s
        source = there["grp"] * subs + there["sub"]
        rows, part = tile_of(source), source % many
        held = sub_iota // block == part
        here = jnp.full((TILE, LANES), -1, jnp.int32)
        for b in range(block):
            tensor = ids[source * rows_dev + my_rank * block + b]
            here = jnp.where(sub_iota == part * block + b, tensor, here)
        row_ids[rows, :] = jnp.where(held, here, row_ids[rows, :])
        sum_w = jnp.zeros((TILE, LANES), jnp.float32)
        sum_u = jnp.zeros((TILE, LANES), jnp.float32)
        for c in range(columns):
            cut = slice(c * LANES, (c + 1) * LANES)

            def arrived(a):
                return jnp.concatenate([landed[k, a, :, cut]] * many, axis=0)

            def put(ref, value):
                ref[rows, cut] = jnp.where(held, value, ref[rows, cut])

            grown = grad[rows, cut]
            w = arrived(0)
            first = beta_one * arrived(1) + (1.0 - beta_one) * grown
            second = beta_two * arrived(2) + (1.0 - beta_two) * grown * grown
            u = (first * scale_one) / (jnp.sqrt(second * scale_two) + adam_eps) + decay_rate * w
            put(first_out, first)
            put(second_out, second)
            put(weights, w)
            put(update, u)
            sum_w += w * w
            sum_u += u * u
        for t in range(LAYERS):
            acc_w[t] += jnp.where(here == t, sum_w, 0.0)
            acc_u[t] += jnp.where(here == t, sum_u, 0.0)

    consume(0, 0)
    for s in take_order:

        def receive(i, carry, s=s):
            g = groups - 1 - i
            exchange(g, s).wait_recv()
            consume(g, s)
            return carry

        lax.fori_loop(0, groups if s else groups - 1, receive, 0)

    col_w = jnp.sum(jnp.sum(acc_w[...], axis=1), axis=1, keepdims=True)
    col_u = jnp.sum(jnp.sum(acc_u[...], axis=1), axis=1, keepdims=True)
    spread = jnp.where(lane_iota == sub_iota, col_w, 0.0) + jnp.where(
        lane_iota == sub_iota + LAYERS, col_u, 0.0
    )
    sums[0] = jnp.sum(spread, axis=0, keepdims=True)
    for k in reversed(peers):
        exchange_sum(k).start()
    for k in peers:
        exchange(k // subs, k % subs).wait_send()
    for k in range(1, devices):
        exchange_sum(k).wait_recv()
    for k in range(1, devices):
        exchange_sum(k).wait_send()
    mine = flips(me, devices)
    total = jnp.zeros((1, LANES), jnp.float32)
    for o in range(devices):
        total = total + sums[mine[o]]
    wide = jnp.broadcast_to(total, (TILE, LANES))
    weight_sq = jnp.sum(jnp.where(lane_iota == sub_iota, wide, 0.0), axis=1, keepdims=True)
    update_sq = jnp.sum(jnp.where(lane_iota == sub_iota + LAYERS, wide, 0.0), axis=1, keepdims=True)
    ratio = learn_rate * (jnp.sqrt(weight_sq) / (jnp.sqrt(update_sq) + trust_eps))
    ratio_out[...] = jnp.broadcast_to(ratio, (TILE, LANES))


def finish(ratio_ref, row_ids, weights, update, first, second,
           fresh_hbm, first_hbm, second_hbm, fresh, fresh_sem, moment_sem):
    rows_dev, width = weights.shape
    columns = width // LANES
    moments = [
        pltpu.make_async_copy(first, first_hbm, moment_sem.at[0]),
        pltpu.make_async_copy(second, second_hbm, moment_sem.at[1]),
    ]
    for move in moments:
        move.start()
    ratio = ratio_ref[...]
    span = rows_dev // PIECES
    moves = []
    for p in range(PIECES):

        def step_rows(s, carry):
            base = pl.multiple_of(p * span + s * TILE, TILE)
            here = row_ids[pl.ds(base, TILE), :]
            step = jnp.zeros((TILE, LANES), jnp.float32)
            for t in range(LAYERS):
                step = jnp.where(here == t, jnp.broadcast_to(ratio[t : t + 1], (TILE, LANES)), step)
            for c in range(columns):
                cut = slice(c * LANES, (c + 1) * LANES)
                rows = pl.ds(base, TILE)
                fresh[rows, cut] = weights[rows, cut] - step * update[rows, cut]
            return carry

        lax.fori_loop(0, span // TILE, step_rows, 0)
        rows = pl.ds(p * span, span)
        moves.append(pltpu.make_async_copy(fresh.at[rows], fresh_hbm.at[rows], fresh_sem.at[p]))
        if p:
            moves[p - 1].start()
    moves[-1].start()
    for move in moves + moments:
        move.wait()


def local(groups, subs, master, moment_one, moment_two, gradient, partner, tensor_of_row):
    rows_dev, width = master.shape
    devices = groups * subs
    block = rows_dev // devices
    whole = jax.ShapeDtypeStruct((rows_dev, width), jnp.float32)
    vmem = pl.BlockSpec(memory_space=pltpu.VMEM)
    hbm = pl.BlockSpec(memory_space=pltpu.HBM)
    slots = (devices, 3, block, width)
    weights, update, first, second, row_ids, ratio = pl.pallas_call(
        functools.partial(kernel, groups, subs),
        out_shape=(
            whole,
            whole,
            whole,
            whole,
            jax.ShapeDtypeStruct((rows_dev, LANES), jnp.int32),
            jax.ShapeDtypeStruct((LAYERS, LANES), jnp.float32),
        ),
        in_specs=[hbm] * 6,
        out_specs=(vmem,) * 6,
        scratch_shapes=[
            pltpu.SMEM(partner.shape, jnp.int32),
            pltpu.SMEM(tensor_of_row.shape, jnp.int32),
        ]
        + [pltpu.VMEM((rows_dev // TILE, TILE, width), jnp.float32)] * 3
        + [
            pltpu.VMEM((rows_dev, width), jnp.float32),
            pltpu.VMEM(slots, jnp.float32),
            pltpu.VMEM(slots, jnp.float32),
            pltpu.VMEM((LAYERS, TILE, LANES), jnp.float32),
            pltpu.VMEM((LAYERS, TILE, LANES), jnp.float32),
            pltpu.VMEM((devices, 1, LANES), jnp.float32),
            pltpu.SemaphoreType.DMA((6,)),
        ]
        + [pltpu.SemaphoreType.DMA((devices,))] * 4,
        compiler_params=pltpu.CompilerParams(
            collective_id=0, has_side_effects=True, vmem_limit_bytes=48 * 1024 * 1024
        ),
    )(
        partner,
        tensor_of_row,
        *(x.reshape(rows_dev // TILE, TILE, width) for x in (master, moment_one, moment_two)),
        gradient,
    )
    return pl.pallas_call(
        finish,
        out_shape=(whole, whole, whole),
        in_specs=[vmem] * 6,
        out_specs=(hbm, hbm, hbm),
        scratch_shapes=[
            pltpu.VMEM((rows_dev, width), jnp.float32),
            pltpu.SemaphoreType.DMA((PIECES,)),
            pltpu.SemaphoreType.DMA((2,)),
        ],
        compiler_params=pltpu.CompilerParams(vmem_limit_bytes=32 * 1024 * 1024),
    )(ratio, row_ids, weights, update, first, second)


def solution(mesh):
    rows = P(("grp", "sub"), None)
    return jax.shard_map(
        functools.partial(local, mesh.shape["grp"], mesh.shape["sub"]),
        mesh=mesh,
        in_specs=(rows, rows, rows, rows, P(), P()),
        out_specs=(rows, rows, rows),
        check_vma=False,
    )
```

```python
import functools

import jax
import jax.numpy as jnp
from jax import lax
from jax.experimental import pallas as pl
from jax.experimental.pallas import tpu as pltpu
from jax.sharding import PartitionSpec as P

LAYERS = 8
LANES = 128
TILE = 8
PIECES = 4
MESH = pl.DeviceIdType.MESH

beta_one = 0.9
beta_two = 0.999
step_count = 10
adam_eps = 1e-06
trust_eps = 1e-06
learn_rate = 0.05
decay_rate = 0.01


def xor(a, b, bound):
    total, bit = 0, 1
    while bit < bound:
        total = total + ((a // bit + b // bit) % 2) * bit
        bit *= 2
    return total


def flips(here, bound):
    steps, bit = [], 1
    while bit < bound:
        steps.append(bit - 2 * bit * ((here // bit) % 2))
        bit *= 2
    return [
        here + sum(step for b, step in enumerate(steps) if (k >> b) % 2) for k in range(bound)
    ]


def sub_order(subs):
    width = subs.bit_length() - 1
    codes = [i ^ (i >> 1) for i in range(subs)]
    return [sum(((c >> b) & 1) << (width - 1 - b) for b in range(width)) for c in codes]


def kernel(groups, subs, partner_hbm, ids_hbm, master_hbm, one_hbm, two_hbm, grad_hbm,
           weights, update, first_out, second_out, row_ids, ratio_out,
           partner, ids, master, one, two, grad, staged, landed, acc_w, acc_u, sums,
           load_sem, send_sem, recv_sem, sum_send, sum_recv):
    devices = groups * subs
    rows_dev, width = grad.shape
    block = rows_dev // devices
    many = TILE // block
    columns = width // LANES
    my_grp, my_sub = lax.axis_index("grp"), lax.axis_index("sub")
    me = my_grp * subs + my_sub
    grps, sbs = flips(my_grp, groups), flips(my_sub, subs)
    order = sub_order(subs)
    send_order = order[1:] + order[:1]
    take_order = [s for s in order if s != subs - 1] + [subs - 1]
    peers = [g * subs + s for s in send_order for g in range(groups) if g or s]

    loads = [
        pltpu.make_async_copy(src, dst, load_sem.at[i])
        for i, (src, dst) in enumerate([
            (partner_hbm, partner), (master_hbm, master), (one_hbm, one), (two_hbm, two),
            (ids_hbm, ids), (grad_hbm, grad),
        ])
    ]
    for load in loads:
        load.start()

    def at(k):
        return {"grp": grps[k // subs], "sub": sbs[k % subs]}

    barrier = pltpu.get_barrier_semaphore()
    for k in reversed(peers):
        pl.semaphore_signal(barrier, inc=1, device_id=at(k), device_id_type=MESH)

    def across(g, s):
        return {"grp": xor(my_grp, g, groups), "sub": xor(my_sub, s, subs)}

    def exchange(g, s):
        there, k = across(g, s), g * subs + s
        return pltpu.make_async_remote_copy(
            src_ref=staged.at[k],
            dst_ref=landed.at[k],
            send_sem=send_sem.at[k],
            recv_sem=recv_sem.at[k],
            device_id=there,
            device_id_type=MESH,
        )

    def exchange_sum(k):
        return pltpu.make_async_remote_copy(
            src_ref=sums.at[0],
            dst_ref=sums.at[k],
            send_sem=sum_send.at[k],
            recv_sem=sum_recv.at[k],
            device_id=at(k),
            device_id_type=MESH,
        )

    def rank_of(device):
        def seek(n, found):
            return jnp.where(partner[n] == device, n, found)

        return lax.fori_loop(0, devices, seek, jnp.int32(0), unroll=8)

    def tile_of(place):
        return pl.ds(pl.multiple_of(place // many * TILE, TILE), TILE)

    loads[0].wait()

    def stage(g, s, target):
        there = across(g, s)
        rank = rank_of(there["grp"] * subs + there["sub"])
        slab, part = rank // many, jnp.full((block, LANES), rank % many, jnp.int32)
        for a, source in enumerate((master, one, two)):
            for c in range(columns):
                cut = slice(c * LANES, (c + 1) * LANES)
                tile = source[slab, :, cut]
                piece = tile[:block]
                for i in range(1, many):
                    piece = jnp.where(part == i, tile[i * block : (i + 1) * block], piece)
                target[a, :, cut] = piece

    for load in loads[1:4]:
        load.wait()
    for s in send_order:
        last = 0 if s else 1
        stage(groups - 1, s, staged.at[(groups - 1) * subs + s])
        if s == send_order[0]:
            pl.semaphore_wait(barrier, devices - 1)

        def send(i, carry, s=s):
            g = groups - 1 - i
            stage(g - 1, s, staged.at[(g - 1) * subs + s])
            exchange(g, s).start()
            return carry

        lax.fori_loop(0, groups - 1 - last, send, 0)
        exchange(last, s).start()
    stage(0, 0, landed.at[0])
    my_rank = rank_of(me)
    loads[4].wait()
    loads[5].wait()
    acc_w[...] = jnp.zeros_like(acc_w)
    acc_u[...] = jnp.zeros_like(acc_u)
    sub_iota = lax.broadcasted_iota(jnp.int32, (TILE, LANES), 0)
    lane_iota = lax.broadcasted_iota(jnp.int32, (TILE, LANES), 1)
    scale_one = 1.0 / (1.0 - beta_one**step_count)
    scale_two = 1.0 / (1.0 - beta_two**step_count)

    def consume(g, s):
        there, k = across(g, s), g * subs + s
        source = there["grp"] * subs + there["sub"]
        rows, part = tile_of(source), source % many
        held = sub_iota // block == part
        here = jnp.full((TILE, LANES), -1, jnp.int32)
        for b in range(block):
            tensor = ids[source * rows_dev + my_rank * block + b]
            here = jnp.where(sub_iota == part * block + b, tensor, here)
        row_ids[rows, :] = jnp.where(held, here, row_ids[rows, :])
        sum_w = jnp.zeros((TILE, LANES), jnp.float32)
        sum_u = jnp.zeros((TILE, LANES), jnp.float32)
        for c in range(columns):
            cut = slice(c * LANES, (c + 1) * LANES)

            def arrived(a):
                return jnp.concatenate([landed[k, a, :, cut]] * many, axis=0)

            def put(ref, value):
                ref[rows, cut] = jnp.where(held, value, ref[rows, cut])

            grown = grad[rows, cut]
            w = arrived(0)
            first = beta_one * arrived(1) + (1.0 - beta_one) * grown
            second = beta_two * arrived(2) + (1.0 - beta_two) * grown * grown
            u = (first * scale_one) / (jnp.sqrt(second * scale_two) + adam_eps) + decay_rate * w
            put(first_out, first)
            put(second_out, second)
            put(weights, w)
            put(update, u)
            sum_w += w * w
            sum_u += u * u
        for t in range(LAYERS):
            acc_w[t] += jnp.where(here == t, sum_w, 0.0)
            acc_u[t] += jnp.where(here == t, sum_u, 0.0)

    consume(0, 0)
    for s in take_order:

        def receive(i, carry, s=s):
            g = groups - 1 - i
            exchange(g, s).wait_recv()
            consume(g, s)
            return carry

        lax.fori_loop(0, groups if s else groups - 1, receive, 0)

    col_w = jnp.sum(jnp.sum(acc_w[...], axis=1), axis=1, keepdims=True)
    col_u = jnp.sum(jnp.sum(acc_u[...], axis=1), axis=1, keepdims=True)
    spread = jnp.where(lane_iota == sub_iota, col_w, 0.0) + jnp.where(
        lane_iota == sub_iota + LAYERS, col_u, 0.0
    )
    sums[0] = jnp.sum(spread, axis=0, keepdims=True)
    for k in reversed(peers):
        exchange_sum(k).start()
    for k in peers:
        exchange(k // subs, k % subs).wait_send()
    for k in range(1, devices):
        exchange_sum(k).wait_recv()
    for k in range(1, devices):
        exchange_sum(k).wait_send()
    mine = flips(me, devices)
    total = jnp.zeros((1, LANES), jnp.float32)
    for o in range(devices):
        total = total + sums[mine[o]]
    wide = jnp.broadcast_to(total, (TILE, LANES))
    weight_sq = jnp.sum(jnp.where(lane_iota == sub_iota, wide, 0.0), axis=1, keepdims=True)
    update_sq = jnp.sum(jnp.where(lane_iota == sub_iota + LAYERS, wide, 0.0), axis=1, keepdims=True)
    ratio = learn_rate * (jnp.sqrt(weight_sq) / (jnp.sqrt(update_sq) + trust_eps))
    ratio_out[...] = jnp.broadcast_to(ratio, (TILE, LANES))


def finish(ratio_ref, row_ids, weights, update, first, second,
           fresh_hbm, first_hbm, second_hbm, fresh, fresh_sem, moment_sem):
    rows_dev, width = weights.shape
    columns = width // LANES
    moments = [
        pltpu.make_async_copy(first, first_hbm, moment_sem.at[0]),
        pltpu.make_async_copy(second, second_hbm, moment_sem.at[1]),
    ]
    for move in moments:
        move.start()
    ratio = ratio_ref[...]
    span = rows_dev // PIECES
    moves = []
    for p in range(PIECES):

        def step_rows(s, carry):
            base = pl.multiple_of(p * span + s * TILE, TILE)
            here = row_ids[pl.ds(base, TILE), :]
            step = jnp.zeros((TILE, LANES), jnp.float32)
            for t in range(LAYERS):
                step = jnp.where(here == t, jnp.broadcast_to(ratio[t : t + 1], (TILE, LANES)), step)
            for c in range(columns):
                cut = slice(c * LANES, (c + 1) * LANES)
                rows = pl.ds(base, TILE)
                fresh[rows, cut] = weights[rows, cut] - step * update[rows, cut]
            return carry

        lax.fori_loop(0, span // TILE, step_rows, 0)
        rows = pl.ds(p * span, span)
        moves.append(pltpu.make_async_copy(fresh.at[rows], fresh_hbm.at[rows], fresh_sem.at[p]))
        if p:
            moves[p - 1].start()
    moves[-1].start()
    for move in moves + moments:
        move.wait()


def local(groups, subs, master, moment_one, moment_two, gradient, partner, tensor_of_row):
    rows_dev, width = master.shape
    devices = groups * subs
    block = rows_dev // devices
    whole = jax.ShapeDtypeStruct((rows_dev, width), jnp.float32)
    vmem = pl.BlockSpec(memory_space=pltpu.VMEM)
    hbm = pl.BlockSpec(memory_space=pltpu.HBM)
    slots = (devices, 3, block, width)
    weights, update, first, second, row_ids, ratio = pl.pallas_call(
        functools.partial(kernel, groups, subs),
        out_shape=(
            *[pltpu.VMEM((rows_dev, width), jnp.float32)] * 4,
            pltpu.VMEM((rows_dev, LANES), jnp.int32),
            pltpu.VMEM((LAYERS, LANES), jnp.float32),
        ),
        in_specs=[hbm] * 6,
        out_specs=(vmem,) * 6,
        scratch_shapes=[
            pltpu.SMEM(partner.shape, jnp.int32),
            pltpu.SMEM(tensor_of_row.shape, jnp.int32),
        ]
        + [pltpu.VMEM((rows_dev // TILE, TILE, width), jnp.float32)] * 3
        + [
            pltpu.VMEM((rows_dev, width), jnp.float32),
            pltpu.VMEM(slots, jnp.float32),
            pltpu.VMEM(slots, jnp.float32),
            pltpu.VMEM((LAYERS, TILE, LANES), jnp.float32),
            pltpu.VMEM((LAYERS, TILE, LANES), jnp.float32),
            pltpu.VMEM((devices, 1, LANES), jnp.float32),
            pltpu.SemaphoreType.DMA((6,)),
        ]
        + [pltpu.SemaphoreType.DMA((devices,))] * 4,
        compiler_params=pltpu.CompilerParams(
            collective_id=0, has_side_effects=True, vmem_limit_bytes=48 * 1024 * 1024
        ),
    )(*(
        pltpu.with_memory_space_constraint(x, pltpu.HBM)
        for x in (
            partner,
            tensor_of_row,
            *(x.reshape(rows_dev // TILE, TILE, width) for x in (master, moment_one, moment_two)),
            gradient,
        )
    ))
    return pl.pallas_call(
        finish,
        out_shape=(whole, whole, whole),
        in_specs=[vmem] * 6,
        out_specs=(hbm, hbm, hbm),
        scratch_shapes=[
            pltpu.VMEM((rows_dev, width), jnp.float32),
            pltpu.SemaphoreType.DMA((PIECES,)),
            pltpu.SemaphoreType.DMA((2,)),
        ],
        compiler_params=pltpu.CompilerParams(vmem_limit_bytes=32 * 1024 * 1024),
    )(ratio, row_ids, weights, update, first, second)


def solution(mesh):
    rows = P(("grp", "sub"), None)
    return jax.shard_map(
        functools.partial(local, mesh.shape["grp"], mesh.shape["sub"]),
        mesh=mesh,
        in_specs=(rows, rows, rows, rows, P(), P()),
        out_specs=(rows, rows, rows),
        check_vma=False,
    )
```

```python
import functools

import jax
import jax.numpy as jnp
from jax import lax
from jax.experimental import pallas as pl
from jax.experimental.pallas import tpu as pltpu
from jax.sharding import PartitionSpec as P

LAYERS = 8
LANES = 128
TILE = 8
PIECES = 4
HELD = 2
MESH = pl.DeviceIdType.MESH

beta_one = 0.9
beta_two = 0.999
step_count = 10
adam_eps = 1e-06
trust_eps = 1e-06
learn_rate = 0.05
decay_rate = 0.01


def xor(a, b, bound):
    total, bit = 0, 1
    while bit < bound:
        total = total + ((a // bit + b // bit) % 2) * bit
        bit *= 2
    return total


def flips(here, bound):
    steps, bit = [], 1
    while bit < bound:
        steps.append(bit - 2 * bit * ((here // bit) % 2))
        bit *= 2
    return [
        here + sum(step for b, step in enumerate(steps) if (k >> b) % 2) for k in range(bound)
    ]


def sub_order(subs):
    width = subs.bit_length() - 1
    codes = [i ^ (i >> 1) for i in range(subs)]
    return [sum(((c >> b) & 1) << (width - 1 - b) for b in range(width)) for c in codes]


def kernel(groups, subs, partner_hbm, ids_hbm, master_hbm, one_hbm, two_hbm, grad_hbm,
           weights, update, first_out, second_out, row_ids, ratio_out,
           partner, ids, master, one, two, grad, staged, landed, acc_w, acc_u, sums,
           near, lent, borrowed, load_sem, send_sem, recv_sem, sum_send, sum_recv,
           near_sem, lend_send, lend_recv):
    devices = groups * subs
    rows_dev, width = grad.shape
    block = rows_dev // devices
    many = TILE // block
    columns = width // LANES
    my_grp, my_sub = lax.axis_index("grp"), lax.axis_index("sub")
    me = my_grp * subs + my_sub
    grps, sbs = flips(my_grp, groups), flips(my_sub, subs)
    order = sub_order(subs)
    send_order = order[1:] + order[:1]
    take_order = [s for s in order if s != subs - 1] + [subs - 1]
    peers = [g * subs + s for s in send_order for g in range(groups) if g or s]
    across_all = subs - 1
    inner = (my_sub == subs // 2 - 1) | (my_sub == subs // 2)
    held_back = range(near.shape[0])

    def tile_of(place):
        return pl.ds(pl.multiple_of(place // many * TILE, TILE), TILE)

    def slot_of(g, s):
        return grps[g] * subs + sbs[s]

    fetches = [
        pltpu.make_async_copy(
            grad_hbm.at[tile_of(slot_of(h, across_all))], near.at[h], near_sem.at[h]
        )
        for h in held_back
    ]
    for fetch in fetches:
        fetch.start()
    loads = [
        pltpu.make_async_copy(src, dst, load_sem.at[i])
        for i, (src, dst) in enumerate([
            (partner_hbm, partner), (master_hbm, master), (one_hbm, one), (two_hbm, two),
            (ids_hbm, ids), (grad_hbm, grad),
        ])
    ]
    for load in loads:
        load.start()

    def at(k):
        return {"grp": grps[k // subs], "sub": sbs[k % subs]}

    barrier = pltpu.get_barrier_semaphore()
    for k in reversed(peers):
        pl.semaphore_signal(barrier, inc=1, device_id=at(k), device_id_type=MESH)

    def across(g, s):
        return {"grp": xor(my_grp, g, groups), "sub": xor(my_sub, s, subs)}

    def exchange(g, s):
        there, k = across(g, s), g * subs + s
        return pltpu.make_async_remote_copy(
            src_ref=staged.at[k],
            dst_ref=landed.at[k],
            send_sem=send_sem.at[k],
            recv_sem=recv_sem.at[k],
            device_id=there,
            device_id_type=MESH,
        )

    def exchange_sum(k):
        return pltpu.make_async_remote_copy(
            src_ref=sums.at[0],
            dst_ref=sums.at[k],
            send_sem=sum_send.at[k],
            recv_sem=sum_recv.at[k],
            device_id=at(k),
            device_id_type=MESH,
        )

    def rank_of(device):
        def seek(n, found):
            return jnp.where(partner[n] == device, n, found)

        return lax.fori_loop(0, devices, seek, jnp.int32(0), unroll=8)

    def lend(h):
        return pltpu.make_async_remote_copy(
            src_ref=lent.at[h],
            dst_ref=borrowed.at[h],
            send_sem=lend_send.at[h],
            recv_sem=lend_recv.at[h],
            device_id=at(h * subs + across_all),
            device_id_type=MESH,
        )

    def cuts():
        return [slice(c * LANES, (c + 1) * LANES) for c in range(columns)]

    def pick(tile, part):
        piece = tile[:block]
        for i in range(1, many):
            piece = jnp.where(part == i, tile[i * block : (i + 1) * block], piece)
        return piece

    for h in held_back:
        fetches[h].wait()
        for cut in cuts():
            lent[h, :, cut] = pick(near[h, :, cut], slot_of(h, across_all) % many)
    loads[0].wait()

    def stage(g, s, target):
        there = across(g, s)
        rank = rank_of(there["grp"] * subs + there["sub"])
        slab, part = rank // many, jnp.full((block, LANES), rank % many, jnp.int32)
        for a, source in enumerate((master, one, two)):
            for cut in cuts():
                target[a, :, cut] = pick(source[slab, :, cut], part)

    pl.semaphore_wait(barrier, devices - 1)

    @pl.when(inner)
    def _():
        for h in held_back:
            lend(h).start()

    for load in loads[1:4]:
        load.wait()
    for s in send_order:
        last = 0 if s else 1
        turn = my_grp % 2 * (groups // 2) if s else 0

        def step(i, turn=turn):
            return xor(groups - 1 - i, turn, groups)

        def send_one(g, s=s):
            if s == across_all:
                pl.when(jnp.logical_not(inner & (g < len(held_back))))(exchange(g, s).start)
            else:
                exchange(g, s).start()

        first_g = step(0)
        stage(first_g, s, staged.at[first_g * subs + s])

        def send(i, carry, s=s, step=step, send_one=send_one):
            g, later = step(i), step(i + 1)
            stage(later, s, staged.at[later * subs + s])
            send_one(g)
            return carry

        lax.fori_loop(0, groups - 1 - last, send, 0)
        send_one(step(groups - 1 - last))

    @pl.when(inner)
    def _():
        for h in held_back[1:]:
            exchange(h, across_all).start()

    stage(0, 0, landed.at[0])
    my_rank = rank_of(me)
    loads[4].wait()
    loads[5].wait()
    acc_w[...] = jnp.zeros_like(acc_w)
    acc_u[...] = jnp.zeros_like(acc_u)
    sub_iota = lax.broadcasted_iota(jnp.int32, (TILE, LANES), 0)
    lane_iota = lax.broadcasted_iota(jnp.int32, (TILE, LANES), 1)
    scale_one = 1.0 / (1.0 - beta_one**step_count)
    scale_two = 1.0 / (1.0 - beta_two**step_count)

    def moments(w, one, two, grown):
        first = beta_one * one + (1.0 - beta_one) * grown
        second = beta_two * two + (1.0 - beta_two) * grown * grown
        u = (first * scale_one) / (jnp.sqrt(second * scale_two) + adam_eps) + decay_rate * w
        return first, second, u

    def name_rows(start, part):
        here = jnp.full((TILE, LANES), -1, jnp.int32)
        for b in range(block):
            here = jnp.where(sub_iota == part * block + b, ids[start + b], here)
        return here

    def account(here, sum_w, sum_u):
        for t in range(LAYERS):
            acc_w[t] += jnp.where(here == t, sum_w, 0.0)
            acc_u[t] += jnp.where(here == t, sum_u, 0.0)

    def consume(g, s, count=True):
        there, k = across(g, s), g * subs + s
        source = there["grp"] * subs + there["sub"]
        rows, part = tile_of(source), source % many
        held = sub_iota // block == part
        here = name_rows(source * rows_dev + my_rank * block, part)
        row_ids[rows, :] = jnp.where(held, here, row_ids[rows, :])
        sum_w = jnp.zeros((TILE, LANES), jnp.float32)
        sum_u = jnp.zeros((TILE, LANES), jnp.float32)
        for cut in cuts():

            def arrived(a):
                return jnp.concatenate([landed[k, a, :, cut]] * many, axis=0)

            def put(ref, value):
                ref[rows, cut] = jnp.where(held, value, ref[rows, cut])

            w = arrived(0)
            first, second, u = moments(w, arrived(1), arrived(2), grad[rows, cut])
            put(first_out, first)
            put(second_out, second)
            put(weights, w)
            put(update, u)
            sum_w += w * w
            sum_u += u * u
        if count:
            account(here, sum_w, sum_u)

    def count_held(h):
        k = h * subs + across_all
        start = me * rows_dev + rank_of(slot_of(h, across_all)) * block
        sum_w = jnp.zeros((block, LANES), jnp.float32)
        sum_u = jnp.zeros((block, LANES), jnp.float32)
        for cut in cuts():
            w = staged[k, 0, :, cut]
            _, _, u = moments(w, staged[k, 1, :, cut], staged[k, 2, :, cut], borrowed[h, :, cut])
            sum_w += w * w
            sum_u += u * u
        account(
            name_rows(start, 0),
            jnp.concatenate([sum_w] * many, axis=0),
            jnp.concatenate([sum_u] * many, axis=0),
        )

    consume(0, 0)
    for s in take_order:
        if s == across_all:

            @pl.when(inner)
            def _():
                for h in held_back:
                    lend(h).wait_recv()
                    count_held(h)

        def receive(i, carry, s=s):
            g = groups - 1 - i

            def take():
                exchange(g, s).wait_recv()
                consume(g, s)

            if s == across_all:
                pl.when(jnp.logical_not(inner & (g < len(held_back))))(take)
            else:
                take()
            return carry

        lax.fori_loop(0, groups if s else groups - 1, receive, 0)

    col_w = jnp.sum(jnp.sum(acc_w[...], axis=1), axis=1, keepdims=True)
    col_u = jnp.sum(jnp.sum(acc_u[...], axis=1), axis=1, keepdims=True)
    spread = jnp.where(lane_iota == sub_iota, col_w, 0.0) + jnp.where(
        lane_iota == sub_iota + LAYERS, col_u, 0.0
    )
    sums[0] = jnp.sum(spread, axis=0, keepdims=True)
    for k in reversed(peers):
        exchange_sum(k).start()

    @pl.when(inner)
    def _():
        exchange(0, across_all).start()

    for k in range(1, devices):
        exchange_sum(k).wait_recv()
    mine = flips(me, devices)
    total = jnp.zeros((1, LANES), jnp.float32)
    for o in range(devices):
        total = total + sums[mine[o]]
    wide = jnp.broadcast_to(total, (TILE, LANES))
    weight_sq = jnp.sum(jnp.where(lane_iota == sub_iota, wide, 0.0), axis=1, keepdims=True)
    update_sq = jnp.sum(jnp.where(lane_iota == sub_iota + LAYERS, wide, 0.0), axis=1, keepdims=True)
    ratio = learn_rate * (jnp.sqrt(weight_sq) / (jnp.sqrt(update_sq) + trust_eps))
    ratio_out[...] = jnp.broadcast_to(ratio, (TILE, LANES))

    @pl.when(inner)
    def _():
        for h in reversed(held_back):
            exchange(h, across_all).wait_recv()
            consume(h, across_all, count=False)
        for h in held_back:
            lend(h).wait_send()

    for k in peers:
        exchange(k // subs, k % subs).wait_send()
    for k in range(1, devices):
        exchange_sum(k).wait_send()


def finish(ratio_ref, row_ids, weights, update, first, second,
           fresh_hbm, first_hbm, second_hbm, fresh, fresh_sem, moment_sem):
    rows_dev, width = weights.shape
    columns = width // LANES
    moments = [
        pltpu.make_async_copy(first, first_hbm, moment_sem.at[0]),
        pltpu.make_async_copy(second, second_hbm, moment_sem.at[1]),
    ]
    for move in moments:
        move.start()
    ratio = ratio_ref[...]
    span = rows_dev // PIECES
    moves = []
    for p in range(PIECES):

        def step_rows(s, carry):
            base = pl.multiple_of(p * span + s * TILE, TILE)
            here = row_ids[pl.ds(base, TILE), :]
            step = jnp.zeros((TILE, LANES), jnp.float32)
            for t in range(LAYERS):
                step = jnp.where(here == t, jnp.broadcast_to(ratio[t : t + 1], (TILE, LANES)), step)
            for c in range(columns):
                cut = slice(c * LANES, (c + 1) * LANES)
                rows = pl.ds(base, TILE)
                fresh[rows, cut] = weights[rows, cut] - step * update[rows, cut]
            return carry

        lax.fori_loop(0, span // TILE, step_rows, 0)
        rows = pl.ds(p * span, span)
        moves.append(pltpu.make_async_copy(fresh.at[rows], fresh_hbm.at[rows], fresh_sem.at[p]))
        if p:
            moves[p - 1].start()
    moves[-1].start()
    for move in moves + moments:
        move.wait()


def local(groups, subs, master, moment_one, moment_two, gradient, partner, tensor_of_row):
    rows_dev, width = master.shape
    devices = groups * subs
    block = rows_dev // devices
    whole = jax.ShapeDtypeStruct((rows_dev, width), jnp.float32)
    vmem = pl.BlockSpec(memory_space=pltpu.VMEM)
    hbm = pl.BlockSpec(memory_space=pltpu.HBM)
    slots = (devices, 3, block, width)
    held_back = min(HELD, groups)
    weights, update, first, second, row_ids, ratio = pl.pallas_call(
        functools.partial(kernel, groups, subs),
        out_shape=(
            *[pltpu.VMEM((rows_dev, width), jnp.float32)] * 4,
            pltpu.VMEM((rows_dev, LANES), jnp.int32),
            pltpu.VMEM((LAYERS, LANES), jnp.float32),
        ),
        in_specs=[hbm] * 6,
        out_specs=(vmem,) * 6,
        scratch_shapes=[
            pltpu.SMEM(partner.shape, jnp.int32),
            pltpu.SMEM(tensor_of_row.shape, jnp.int32),
        ]
        + [pltpu.VMEM((rows_dev // TILE, TILE, width), jnp.float32)] * 3
        + [
            pltpu.VMEM((rows_dev, width), jnp.float32),
            pltpu.VMEM(slots, jnp.float32),
            pltpu.VMEM(slots, jnp.float32),
            pltpu.VMEM((LAYERS, TILE, LANES), jnp.float32),
            pltpu.VMEM((LAYERS, TILE, LANES), jnp.float32),
            pltpu.VMEM((devices, 1, LANES), jnp.float32),
            pltpu.VMEM((held_back, TILE, width), jnp.float32),
            pltpu.VMEM((held_back, block, width), jnp.float32),
            pltpu.VMEM((held_back, block, width), jnp.float32),
            pltpu.SemaphoreType.DMA((6,)),
        ]
        + [pltpu.SemaphoreType.DMA((devices,))] * 4
        + [pltpu.SemaphoreType.DMA((held_back,))] * 3,
        compiler_params=pltpu.CompilerParams(
            collective_id=0, has_side_effects=True, vmem_limit_bytes=48 * 1024 * 1024
        ),
    )(*(
        pltpu.with_memory_space_constraint(x, pltpu.HBM)
        for x in (
            partner,
            tensor_of_row,
            *(x.reshape(rows_dev // TILE, TILE, width) for x in (master, moment_one, moment_two)),
            gradient,
        )
    ))
    return pl.pallas_call(
        finish,
        out_shape=(whole, whole, whole),
        in_specs=[vmem] * 6,
        out_specs=(hbm, hbm, hbm),
        scratch_shapes=[
            pltpu.VMEM((rows_dev, width), jnp.float32),
            pltpu.SemaphoreType.DMA((PIECES,)),
            pltpu.SemaphoreType.DMA((2,)),
        ],
        compiler_params=pltpu.CompilerParams(vmem_limit_bytes=32 * 1024 * 1024),
    )(ratio, row_ids, weights, update, first, second)


def solution(mesh):
    rows = P(("grp", "sub"), None)
    return jax.shard_map(
        functools.partial(local, mesh.shape["grp"], mesh.shape["sub"]),
        mesh=mesh,
        in_specs=(rows, rows, rows, rows, P(), P()),
        out_specs=(rows, rows, rows),
        check_vma=False,
    )
```

```python
import functools

import jax
import jax.numpy as jnp
from jax import lax
from jax.experimental import pallas as pl
from jax.experimental.pallas import tpu as pltpu
from jax.sharding import PartitionSpec as P

LAYERS = 8
LANES = 128
TILE = 8
PIECES = 4
HELD = 2
MESH = pl.DeviceIdType.MESH

beta_one = 0.9
beta_two = 0.999
step_count = 10
adam_eps = 1e-06
trust_eps = 1e-06
learn_rate = 0.05
decay_rate = 0.01


def xor(a, b, bound):
    total, bit = 0, 1
    while bit < bound:
        total = total + ((a // bit + b // bit) % 2) * bit
        bit *= 2
    return total


def flips(here, bound):
    steps, bit = [], 1
    while bit < bound:
        steps.append(bit - 2 * bit * ((here // bit) % 2))
        bit *= 2
    return [
        here + sum(step for b, step in enumerate(steps) if (k >> b) % 2) for k in range(bound)
    ]


def sub_order(subs):
    width = subs.bit_length() - 1
    codes = [i ^ (i >> 1) for i in range(subs)]
    return [sum(((c >> b) & 1) << (width - 1 - b) for b in range(width)) for c in codes]


def kernel(groups, subs, partner_hbm, ids_hbm, master_hbm, one_hbm, two_hbm, grad_hbm,
           weights, update, first_out, second_out, row_ids, ratio_out,
           partner, ids, master, one, two, grad, staged, landed, acc_w, acc_u, sums,
           near, lent, borrowed, near_sem, partner_sem, ids_sem, grad_sem, send_sem,
           sum_send, sum_recv, lend_send, lend_recv, load_sem, recv_sem):
    devices = groups * subs
    rows_dev, width = grad.shape
    block = rows_dev // devices
    many = TILE // block
    columns = width // LANES
    my_grp, my_sub = lax.axis_index("grp"), lax.axis_index("sub")
    me = my_grp * subs + my_sub
    grps, sbs = flips(my_grp, groups), flips(my_sub, subs)
    order = sub_order(subs)
    send_order = order[1:] + order[:1]
    take_order = [s for s in order if s != subs - 1] + [subs - 1]
    peers = [(g, s) for s in send_order for g in range(groups) if g or s]
    across_all = subs - 1
    inner = (my_sub == subs // 2 - 1) | (my_sub == subs // 2)
    held_back = range(near.shape[0])

    def tile_of(place):
        return pl.ds(pl.multiple_of(place // many * TILE, TILE), TILE)

    def device_of(g, s):
        return grps[g] * subs + sbs[s]

    for h in held_back:
        pltpu.make_async_copy(
            grad_hbm.at[tile_of(device_of(h, across_all))], near.at[h], near_sem
        ).start()
    pltpu.make_async_copy(partner_hbm, partner, partner_sem).start()

    def at(g, s):
        return {"grp": grps[g], "sub": sbs[s]}

    barrier = pltpu.get_barrier_semaphore()
    for g, s in peers:
        pl.semaphore_signal(barrier, inc=1, device_id=at(g, s), device_id_type=MESH)

    def across(g, s):
        return {"grp": xor(my_grp, g, groups), "sub": xor(my_sub, s, subs)}

    def exchange(g, s):
        k = s * groups + g
        return pltpu.make_async_remote_copy(
            src_ref=staged.at[k],
            dst_ref=landed.at[k],
            send_sem=send_sem,
            recv_sem=arrival(g, s),
            device_id=across(g, s),
            device_id_type=MESH,
        )

    def arrival(g, s):
        return recv_sem.at[subs + g] if s == across_all else recv_sem.at[s]

    def batch(s, count):
        run = pl.ds(s * groups + groups - count, count)
        return pltpu.make_async_remote_copy(
            src_ref=staged.at[run],
            dst_ref=landed.at[run],
            send_sem=send_sem,
            recv_sem=recv_sem.at[s % subs],
            device_id=at(1, 0),
            device_id_type=MESH,
        )

    def exchange_sum(g, s):
        return pltpu.make_async_remote_copy(
            src_ref=sums.at[0],
            dst_ref=sums.at[s * groups + g],
            send_sem=sum_send,
            recv_sem=sum_recv,
            device_id=at(g, s),
            device_id_type=MESH,
        )

    def rank_of(device):
        def seek(n, found):
            return jnp.where(partner[n] == device, n, found)

        return lax.fori_loop(0, devices, seek, jnp.int32(0), unroll=8)

    def lend(h):
        return pltpu.make_async_remote_copy(
            src_ref=lent.at[h],
            dst_ref=borrowed.at[h],
            send_sem=lend_send,
            recv_sem=lend_recv,
            device_id=at(h, across_all),
            device_id_type=MESH,
        )

    def cuts():
        return [slice(c * LANES, (c + 1) * LANES) for c in range(columns)]

    def pick(tile, part):
        piece = tile[:block]
        for i in range(1, many):
            piece = jnp.where(part == i, tile[i * block : (i + 1) * block], piece)
        return piece

    pltpu.make_async_copy(near, near, near_sem).wait()
    loads = [
        pltpu.make_async_copy(src, dst, sem)
        for src, dst, sem in [
            (master_hbm, master, load_sem.at[0]), (one_hbm, one, load_sem.at[1]),
            (two_hbm, two, load_sem.at[2]), (ids_hbm, ids, ids_sem), (grad_hbm, grad, grad_sem),
        ]
    ]
    for load in loads:
        load.start()
    for h in held_back:
        for cut in cuts():
            lent[h, :, cut] = pick(near[h, :, cut], device_of(h, across_all) % many)
    pltpu.make_async_copy(partner_hbm, partner, partner_sem).wait()

    def stage(g, s, target):
        there = across(g, s)
        rank = rank_of(there["grp"] * subs + there["sub"])
        slab, part = rank // many, jnp.full((block, LANES), rank % many, jnp.int32)
        for a, source in enumerate((master, one, two)):
            for cut in cuts():
                target[a, :, cut] = pick(source[slab, :, cut], part)

    pl.semaphore_wait(barrier, devices - 1)

    @pl.when(inner)
    def _():
        for h in held_back:
            lend(h).start()

    for load in loads[:3]:
        load.wait()
    for s in send_order:
        last = 0 if s else 1
        turn = my_grp % 2 * (groups // 2) if s else 0

        def step(i, turn=turn):
            return xor(groups - 1 - i, turn, groups)

        def send_one(g, s=s):
            if s == across_all:
                pl.when(jnp.logical_not(inner & (g < len(held_back))))(exchange(g, s).start)
            else:
                exchange(g, s).start()

        first_g = step(0)
        stage(first_g, s, staged.at[s * groups + first_g])

        def send(i, carry, s=s, step=step, send_one=send_one):
            g, later = step(i), step(i + 1)
            stage(later, s, staged.at[s * groups + later])
            send_one(g)
            return carry

        lax.fori_loop(0, groups - 1 - last, send, 0)
        send_one(step(groups - 1 - last))

    @pl.when(inner)
    def _():
        for h in held_back[1:]:
            exchange(h, across_all).start()

    stage(0, 0, landed.at[0])
    my_rank = rank_of(me)
    for load in loads[3:]:
        load.wait()
    acc_w[...] = jnp.zeros_like(acc_w)
    acc_u[...] = jnp.zeros_like(acc_u)
    sub_iota = lax.broadcasted_iota(jnp.int32, (TILE, LANES), 0)
    lane_iota = lax.broadcasted_iota(jnp.int32, (TILE, LANES), 1)
    scale_one = 1.0 / (1.0 - beta_one**step_count)
    scale_two = 1.0 / (1.0 - beta_two**step_count)

    def moments(w, one, two, grown):
        first = beta_one * one + (1.0 - beta_one) * grown
        second = beta_two * two + (1.0 - beta_two) * grown * grown
        u = (first * scale_one) / (jnp.sqrt(second * scale_two) + adam_eps) + decay_rate * w
        return first, second, u

    def name_rows(start, part):
        here = jnp.full((TILE, LANES), -1, jnp.int32)
        for b in range(block):
            here = jnp.where(sub_iota == part * block + b, ids[start + b], here)
        return here

    def account(here, sum_w, sum_u):
        for t in range(LAYERS):
            acc_w[t] += jnp.where(here == t, sum_w, 0.0)
            acc_u[t] += jnp.where(here == t, sum_u, 0.0)

    def consume(g, s, count=True):
        there, k = across(g, s), s * groups + g
        source = there["grp"] * subs + there["sub"]
        rows, part = tile_of(source), source % many
        held = sub_iota // block == part
        here = name_rows(source * rows_dev + my_rank * block, part)
        row_ids[rows, :] = jnp.where(held, here, row_ids[rows, :])
        sum_w = jnp.zeros((TILE, LANES), jnp.float32)
        sum_u = jnp.zeros((TILE, LANES), jnp.float32)
        for cut in cuts():

            def arrived(a):
                return jnp.concatenate([landed[k, a, :, cut]] * many, axis=0)

            def put(ref, value):
                ref[rows, cut] = jnp.where(held, value, ref[rows, cut])

            w = arrived(0)
            first, second, u = moments(w, arrived(1), arrived(2), grad[rows, cut])
            put(first_out, first)
            put(second_out, second)
            put(weights, w)
            put(update, u)
            sum_w += w * w
            sum_u += u * u
        if count:
            account(here, sum_w, sum_u)

    def count_held(h):
        k = across_all * groups + h
        start = me * rows_dev + rank_of(device_of(h, across_all)) * block
        sum_w = jnp.zeros((block, LANES), jnp.float32)
        sum_u = jnp.zeros((block, LANES), jnp.float32)
        for cut in cuts():
            w = staged[k, 0, :, cut]
            _, _, u = moments(w, staged[k, 1, :, cut], staged[k, 2, :, cut], borrowed[h, :, cut])
            sum_w += w * w
            sum_u += u * u
        account(
            name_rows(start, 0),
            jnp.concatenate([sum_w] * many, axis=0),
            jnp.concatenate([sum_u] * many, axis=0),
        )

    consume(0, 0)
    for s in take_order:
        if s == across_all:

            @pl.when(inner)
            def _():
                pltpu.make_async_remote_copy(
                    src_ref=lent,
                    dst_ref=borrowed,
                    send_sem=lend_send,
                    recv_sem=lend_recv,
                    device_id=at(0, across_all),
                    device_id_type=MESH,
                ).wait()
                for h in held_back:
                    count_held(h)

        else:
            batch(s, groups if s else groups - 1).wait_recv()

        def receive(i, carry, s=s):
            g = groups - 1 - i

            def take():
                exchange(g, s).wait_recv()
                consume(g, s)

            if s == across_all:
                pl.when(jnp.logical_not(inner & (g < len(held_back))))(take)
            else:
                consume(g, s)
            return carry

        lax.fori_loop(0, groups if s else groups - 1, receive, 0)

    col_w = jnp.sum(jnp.sum(acc_w[...], axis=1), axis=1, keepdims=True)
    col_u = jnp.sum(jnp.sum(acc_u[...], axis=1), axis=1, keepdims=True)
    spread = jnp.where(lane_iota == sub_iota, col_w, 0.0) + jnp.where(
        lane_iota == sub_iota + LAYERS, col_u, 0.0
    )
    sums[0] = jnp.sum(spread, axis=0, keepdims=True)
    for g, s in peers:
        exchange_sum(g, s).start()

    @pl.when(inner)
    def _():
        exchange(0, across_all).start()

    told = pltpu.make_async_remote_copy(
        src_ref=sums.at[pl.ds(1, devices - 1)],
        dst_ref=sums.at[pl.ds(1, devices - 1)],
        send_sem=sum_send,
        recv_sem=sum_recv,
        device_id=at(1, 0),
        device_id_type=MESH,
    )
    told.wait_recv()
    total = jnp.zeros((1, LANES), jnp.float32)
    for g in range(groups):
        for s in range(subs):
            total = total + sums[sbs[s] * groups + grps[g]]
    wide = jnp.broadcast_to(total, (TILE, LANES))
    weight_sq = jnp.sum(jnp.where(lane_iota == sub_iota, wide, 0.0), axis=1, keepdims=True)
    update_sq = jnp.sum(jnp.where(lane_iota == sub_iota + LAYERS, wide, 0.0), axis=1, keepdims=True)
    ratio = learn_rate * (jnp.sqrt(weight_sq) / (jnp.sqrt(update_sq) + trust_eps))
    ratio_out[...] = jnp.broadcast_to(ratio, (TILE, LANES))

    @pl.when(inner)
    def _():
        for h in reversed(held_back):
            exchange(h, across_all).wait_recv()
            consume(h, across_all, count=False)

    pltpu.make_async_remote_copy(
        src_ref=staged.at[pl.ds(1, devices - 1)],
        dst_ref=landed.at[pl.ds(1, devices - 1)],
        send_sem=send_sem,
        recv_sem=sum_recv,
        device_id=at(1, 0),
        device_id_type=MESH,
    ).wait_send()
    told.wait_send()


def finish(ratio_ref, row_ids, weights, update, first, second,
           fresh_hbm, first_hbm, second_hbm, fresh, fresh_sem, moment_sem):
    rows_dev, width = weights.shape
    columns = width // LANES
    moments = [
        pltpu.make_async_copy(first, first_hbm, moment_sem.at[0]),
        pltpu.make_async_copy(second, second_hbm, moment_sem.at[1]),
    ]
    for move in moments:
        move.start()
    ratio = ratio_ref[...]
    span = rows_dev // PIECES
    moves = []
    for p in range(PIECES):

        def step_rows(s, carry):
            base = pl.multiple_of(p * span + s * TILE, TILE)
            here = row_ids[pl.ds(base, TILE), :]
            step = jnp.zeros((TILE, LANES), jnp.float32)
            for t in range(LAYERS):
                step = jnp.where(here == t, jnp.broadcast_to(ratio[t : t + 1], (TILE, LANES)), step)
            for c in range(columns):
                cut = slice(c * LANES, (c + 1) * LANES)
                rows = pl.ds(base, TILE)
                fresh[rows, cut] = weights[rows, cut] - step * update[rows, cut]
            return carry

        lax.fori_loop(0, span // TILE, step_rows, 0)
        rows = pl.ds(p * span, span)
        moves.append(pltpu.make_async_copy(fresh.at[rows], fresh_hbm.at[rows], fresh_sem.at[p]))
        if p:
            moves[p - 1].start()
    moves[-1].start()
    for move in moves + moments:
        move.wait()


def local(groups, subs, master, moment_one, moment_two, gradient, partner, tensor_of_row):
    rows_dev, width = master.shape
    devices = groups * subs
    block = rows_dev // devices
    whole = jax.ShapeDtypeStruct((rows_dev, width), jnp.float32)
    vmem = pl.BlockSpec(memory_space=pltpu.VMEM)
    hbm = pl.BlockSpec(memory_space=pltpu.HBM)
    slots = (devices, 3, block, width)
    held_back = min(HELD, groups)
    weights, update, first, second, row_ids, ratio = pl.pallas_call(
        functools.partial(kernel, groups, subs),
        out_shape=(
            *[pltpu.VMEM((rows_dev, width), jnp.float32)] * 4,
            pltpu.VMEM((rows_dev, LANES), jnp.int32),
            pltpu.VMEM((LAYERS, LANES), jnp.float32),
        ),
        in_specs=[hbm] * 6,
        out_specs=(vmem,) * 6,
        scratch_shapes=[
            pltpu.SMEM(partner.shape, jnp.int32),
            pltpu.SMEM(tensor_of_row.shape, jnp.int32),
        ]
        + [pltpu.VMEM((rows_dev // TILE, TILE, width), jnp.float32)] * 3
        + [
            pltpu.VMEM((rows_dev, width), jnp.float32),
            pltpu.VMEM(slots, jnp.float32),
            pltpu.VMEM(slots, jnp.float32),
            pltpu.VMEM((LAYERS, TILE, LANES), jnp.float32),
            pltpu.VMEM((LAYERS, TILE, LANES), jnp.float32),
            pltpu.VMEM((devices, 1, LANES), jnp.float32),
            pltpu.VMEM((held_back, TILE, width), jnp.float32),
            pltpu.VMEM((held_back, block, width), jnp.float32),
            pltpu.VMEM((held_back, block, width), jnp.float32),
        ]
        + [pltpu.SemaphoreType.DMA] * 9
        + [pltpu.SemaphoreType.DMA((3,)), pltpu.SemaphoreType.DMA((subs + groups,))],
        compiler_params=pltpu.CompilerParams(
            collective_id=0, has_side_effects=True, vmem_limit_bytes=48 * 1024 * 1024
        ),
    )(*(
        pltpu.with_memory_space_constraint(x, pltpu.HBM)
        for x in (
            partner,
            tensor_of_row,
            *(x.reshape(rows_dev // TILE, TILE, width) for x in (master, moment_one, moment_two)),
            gradient,
        )
    ))
    return pl.pallas_call(
        finish,
        out_shape=(whole, whole, whole),
        in_specs=[vmem] * 6,
        out_specs=(hbm, hbm, hbm),
        scratch_shapes=[
            pltpu.VMEM((rows_dev, width), jnp.float32),
            pltpu.SemaphoreType.DMA((PIECES,)),
            pltpu.SemaphoreType.DMA((2,)),
        ],
        compiler_params=pltpu.CompilerParams(vmem_limit_bytes=32 * 1024 * 1024),
    )(ratio, row_ids, weights, update, first, second)


def solution(mesh):
    rows = P(("grp", "sub"), None)
    return jax.shard_map(
        functools.partial(local, mesh.shape["grp"], mesh.shape["sub"]),
        mesh=mesh,
        in_specs=(rows, rows, rows, rows, P(), P()),
        out_specs=(rows, rows, rows),
        check_vma=False,
    )
```

```python
import functools

import jax
import jax.numpy as jnp
from jax import lax
from jax.experimental import pallas as pl
from jax.experimental.pallas import tpu as pltpu
from jax.sharding import PartitionSpec as P

LAYERS = 8
LANES = 128
TILE = 8
PIECES = 4
HELD = (2, 2)
AHEAD = (2, 2)
MESH = pl.DeviceIdType.MESH

beta_one = 0.9
beta_two = 0.999
step_count = 10
adam_eps = 1e-06
trust_eps = 1e-06
learn_rate = 0.05
decay_rate = 0.01


def xor(a, b, bound):
    total, bit = 0, 1
    while bit < bound:
        total = total + ((a // bit + b // bit) % 2) * bit
        bit *= 2
    return total


def flips(here, bound):
    steps, bit = [], 1
    while bit < bound:
        steps.append(bit - 2 * bit * ((here // bit) % 2))
        bit *= 2
    return [
        here + sum(step for b, step in enumerate(steps) if (k >> b) % 2) for k in range(bound)
    ]


def sub_order(subs):
    width = subs.bit_length() - 1
    codes = [i ^ (i >> 1) for i in range(subs)]
    return [sum(((c >> b) & 1) << (width - 1 - b) for b in range(width)) for c in codes]


def near_links(groups, subs):
    bits = [1 << b for b in range(subs.bit_length() - 1)]
    flat = [(1 << b, 0) for b in range(groups.bit_length() - 1)]
    flat += [(0, bit) for bit in (bits if subs != 4 else bits[:1])]
    return flat, [(g, subs - 1) for g in range(2) if (g, subs - 1) not in flat]


def diameter(groups, subs):
    return groups.bit_length() - 1 + (3 if subs == 4 else subs.bit_length() - 1)


def kernel(groups, subs, partner_hbm, ids_hbm, master_hbm, one_hbm, two_hbm, grad_hbm,
           weights, update, first_out, second_out, row_ids, ratio_out,
           partner, ids, master, one, two, grad, staged, landed, acc_w, acc_u, sums,
           near, lent, borrowed, rounds, near_sem, partner_sem, ids_sem, grad_sem, send_sem,
           sum_send, sum_recv, lend_send, lend_recv, load_sem, recv_sem):
    devices = groups * subs
    rows_dev, width = grad.shape
    block = rows_dev // devices
    many = TILE // block
    columns = width // LANES
    my_grp, my_sub = lax.axis_index("grp"), lax.axis_index("sub")
    me = my_grp * subs + my_sub
    grps, sbs = flips(my_grp, groups), flips(my_sub, subs)
    order = sub_order(subs)
    send_order = order[1:] + order[:1]
    take_order = [s for s in order if s != subs - 1] + [subs - 1]
    peers = [(g, s) for s in send_order for g in range(groups) if g or s]
    across_all = subs - 1
    inner = (my_sub == subs // 2 - 1) | (my_sub == subs // 2)
    held_back = range(near.shape[0])
    odd = my_grp % 2

    def by_core(pair, core):
        return pair[0] + (pair[1] - pair[0]) * core

    def i_hold(g):
        return inner & (g < by_core(HELD, odd))

    def peer_holds(g):
        return inner & (g < by_core(HELD, (odd + g) % 2))

    def send_held(before):
        ahead = by_core(AHEAD, odd)
        for h in reversed(held_back):
            for a in range(3):
                turn = (by_core(HELD, odd) - 1 - h) * 3 + a
                now = turn < ahead if before else turn >= ahead
                pl.when(i_hold(h) & now)(exchange_array(h, across_all, a).start)

    def tile_of(place):
        return pl.ds(pl.multiple_of(place // many * TILE, TILE), TILE)

    def device_of(g, s):
        return grps[g] * subs + sbs[s]

    for h in held_back:
        pltpu.make_async_copy(
            grad_hbm.at[tile_of(device_of(h, across_all))], near.at[h], near_sem
        ).start()
    pltpu.make_async_copy(partner_hbm, partner, partner_sem).start()

    def at(g, s):
        return {"grp": grps[g], "sub": sbs[s]}

    flat, steep = near_links(groups, subs)
    early = min(2, rounds.shape[0])

    def greet(sem):
        for g, s in flat:
            pl.semaphore_signal(sem, inc=1, device_id=at(g, s), device_id_type=MESH)

        @pl.when(inner)
        def _():
            for g, s in steep:
                pl.semaphore_signal(sem, inc=1, device_id=at(g, s), device_id_type=MESH)

    def hear(sem):
        @pl.when(inner)
        def _():
            pl.semaphore_wait(sem, len(flat) + len(steep))

        @pl.when(jnp.logical_not(inner))
        def _():
            pl.semaphore_wait(sem, len(flat))

    barrier = pltpu.get_barrier_semaphore()
    greet(barrier)

    def across(g, s):
        return {"grp": xor(my_grp, g, groups), "sub": xor(my_sub, s, subs)}

    def exchange(g, s):
        k = s * groups + g
        return pltpu.make_async_remote_copy(
            src_ref=staged.at[k],
            dst_ref=landed.at[k],
            send_sem=send_sem,
            recv_sem=arrival(g, s),
            device_id=across(g, s),
            device_id_type=MESH,
        )

    def exchange_array(g, s, a):
        k = s * groups + g
        return pltpu.make_async_remote_copy(
            src_ref=staged.at[k, a],
            dst_ref=landed.at[k, a],
            send_sem=send_sem,
            recv_sem=arrival(g, s),
            device_id=across(g, s),
            device_id_type=MESH,
        )

    def arrival(g, s):
        return recv_sem.at[subs + g] if s == across_all else recv_sem.at[s]

    def batch(s, count):
        run = pl.ds(s * groups + groups - count, count)
        return pltpu.make_async_remote_copy(
            src_ref=staged.at[run],
            dst_ref=landed.at[run],
            send_sem=send_sem,
            recv_sem=recv_sem.at[s % subs],
            device_id=at(1, 0),
            device_id_type=MESH,
        )

    def exchange_sum(g, s):
        return pltpu.make_async_remote_copy(
            src_ref=sums.at[0],
            dst_ref=sums.at[s * groups + g],
            send_sem=sum_send,
            recv_sem=sum_recv,
            device_id=at(g, s),
            device_id_type=MESH,
        )

    def rank_of(device):
        def seek(n, found):
            return jnp.where(partner[n] == device, n, found)

        return lax.fori_loop(0, devices, seek, jnp.int32(0), unroll=8)

    def lend(h):
        return pltpu.make_async_remote_copy(
            src_ref=lent.at[h],
            dst_ref=borrowed.at[h],
            send_sem=lend_send.at[h],
            recv_sem=lend_recv.at[h],
            device_id=at(h, across_all),
            device_id_type=MESH,
        )

    def cuts():
        return [slice(c * LANES, (c + 1) * LANES) for c in range(columns)]

    def pick(tile, part):
        piece = tile[:block]
        for i in range(1, many):
            piece = jnp.where(part == i, tile[i * block : (i + 1) * block], piece)
        return piece

    pltpu.make_async_copy(near, near, near_sem).wait()
    loads = [
        pltpu.make_async_copy(src, dst, sem)
        for src, dst, sem in [
            (master_hbm, master, load_sem.at[0]), (one_hbm, one, load_sem.at[1]),
            (two_hbm, two, load_sem.at[2]), (ids_hbm, ids, ids_sem), (grad_hbm, grad, grad_sem),
        ]
    ]
    for load in loads[:3]:
        load.start()
    for h in held_back:
        for cut in cuts():
            lent[h, :, cut] = pick(near[h, :, cut], device_of(h, across_all) % many)
    pltpu.make_async_copy(partner_hbm, partner, partner_sem).wait()

    def stage(g, s, target):
        there = across(g, s)
        rank = rank_of(there["grp"] * subs + there["sub"])
        slab, part = rank // many, jnp.full((block, LANES), rank % many, jnp.int32)
        for a, source in enumerate((master, one, two)):
            for cut in cuts():
                target[a, :, cut] = pick(source[slab, :, cut], part)

    hear(barrier)
    for h in held_back:
        pl.when(peer_holds(h))(lend(h).start)

    for r in range(early):
        greet(rounds.at[r])
        hear(rounds.at[r])
    if early < rounds.shape[0]:
        greet(rounds.at[early])
    for load in loads[:3]:
        load.wait()
    for load in loads[3:]:
        load.start()
    for g in range(2):
        stage(g, send_order[0], staged.at[send_order[0] * groups + g])
    for g in range(2):
        exchange(g, send_order[0]).start()
    for r in range(early, rounds.shape[0]):
        hear(rounds.at[r])
        if r + 1 < rounds.shape[0]:
            greet(rounds.at[r + 1])
    for s in send_order:
        begin = 2 if s == send_order[0] else 0 if s else 1
        if begin == groups:
            continue

        def step(i, s=s, begin=begin):
            if s == send_order[0]:
                return 2 + (groups - 3 - i + odd * 4) % (groups - 2)
            return xor(groups - 1 - i, odd * (groups // 2), groups) if s else groups - 1 - i

        def send_one(g, s=s):
            if s == across_all:
                pl.when(jnp.logical_not(i_hold(g)))(exchange(g, s).start)
            else:
                exchange(g, s).start()

        first_g = step(0)
        stage(first_g, s, staged.at[s * groups + first_g])

        def send(i, carry, s=s, step=step, send_one=send_one):
            g, later = step(i), step(i + 1)
            stage(later, s, staged.at[s * groups + later])
            send_one(g)
            return carry

        lax.fori_loop(0, groups - 1 - begin, send, 0)
        send_one(step(groups - 1 - begin))

    send_held(True)

    stage(0, 0, landed.at[0])
    my_rank = rank_of(me)
    for load in loads[3:]:
        load.wait()
    acc_w[...] = jnp.zeros_like(acc_w)
    acc_u[...] = jnp.zeros_like(acc_u)
    sub_iota = lax.broadcasted_iota(jnp.int32, (TILE, LANES), 0)
    lane_iota = lax.broadcasted_iota(jnp.int32, (TILE, LANES), 1)
    scale_one = 1.0 / (1.0 - beta_one**step_count)
    scale_two = 1.0 / (1.0 - beta_two**step_count)

    def moments(w, one, two, grown):
        first = beta_one * one + (1.0 - beta_one) * grown
        second = beta_two * two + (1.0 - beta_two) * grown * grown
        u = (first * scale_one) / (jnp.sqrt(second * scale_two) + adam_eps) + decay_rate * w
        return first, second, u

    def name_rows(start, part):
        here = jnp.full((TILE, LANES), -1, jnp.int32)
        for b in range(block):
            here = jnp.where(sub_iota == part * block + b, ids[start + b], here)
        return here

    def account(here, sum_w, sum_u):
        for t in range(LAYERS):
            acc_w[t] += jnp.where(here == t, sum_w, 0.0)
            acc_u[t] += jnp.where(here == t, sum_u, 0.0)

    def consume(g, s, count=True):
        there, k = across(g, s), s * groups + g
        source = there["grp"] * subs + there["sub"]
        rows, part = tile_of(source), source % many
        held = sub_iota // block == part
        here = name_rows(source * rows_dev + my_rank * block, part)
        row_ids[rows, :] = jnp.where(held, here, row_ids[rows, :])
        sum_w = jnp.zeros((TILE, LANES), jnp.float32)
        sum_u = jnp.zeros((TILE, LANES), jnp.float32)
        for cut in cuts():

            def arrived(a):
                return jnp.concatenate([landed[k, a, :, cut]] * many, axis=0)

            def put(ref, value):
                ref[rows, cut] = jnp.where(held, value, ref[rows, cut])

            w = arrived(0)
            first, second, u = moments(w, arrived(1), arrived(2), grad[rows, cut])
            put(first_out, first)
            put(second_out, second)
            put(weights, w)
            put(update, u)
            sum_w += w * w
            sum_u += u * u
        if count:
            account(here, sum_w, sum_u)

    def count_held(h):
        k = across_all * groups + h
        start = me * rows_dev + rank_of(device_of(h, across_all)) * block
        sum_w = jnp.zeros((block, LANES), jnp.float32)
        sum_u = jnp.zeros((block, LANES), jnp.float32)
        for cut in cuts():
            w = staged[k, 0, :, cut]
            _, _, u = moments(w, staged[k, 1, :, cut], staged[k, 2, :, cut], borrowed[h, :, cut])
            sum_w += w * w
            sum_u += u * u
        account(
            name_rows(start, 0),
            jnp.concatenate([sum_w] * many, axis=0),
            jnp.concatenate([sum_u] * many, axis=0),
        )

    consume(0, 0)
    for s in take_order:
        if s == across_all:

            for h in held_back:

                @pl.when(i_hold(h))
                def _(h=h):
                    lend(h).wait_recv()
                    count_held(h)

        else:
            batch(s, groups if s else groups - 1).wait_recv()

        def receive(i, carry, s=s):
            g = groups - 1 - i

            def take():
                exchange(g, s).wait_recv()
                consume(g, s)

            if s == across_all:
                pl.when(jnp.logical_not(peer_holds(g)))(take)
            else:
                consume(g, s)
            return carry

        lax.fori_loop(0, groups if s else groups - 1, receive, 0)

    col_w = jnp.sum(jnp.sum(acc_w[...], axis=1), axis=1, keepdims=True)
    col_u = jnp.sum(jnp.sum(acc_u[...], axis=1), axis=1, keepdims=True)
    spread = jnp.where(lane_iota == sub_iota, col_w, 0.0) + jnp.where(
        lane_iota == sub_iota + LAYERS, col_u, 0.0
    )
    sums[0] = jnp.sum(spread, axis=0, keepdims=True)
    for g, s in peers:
        exchange_sum(g, s).start()

    send_held(False)

    told = pltpu.make_async_remote_copy(
        src_ref=sums.at[pl.ds(1, devices - 1)],
        dst_ref=sums.at[pl.ds(1, devices - 1)],
        send_sem=sum_send,
        recv_sem=sum_recv,
        device_id=at(1, 0),
        device_id_type=MESH,
    )
    told.wait_recv()
    total = jnp.zeros((1, LANES), jnp.float32)
    for g in range(groups):
        for s in range(subs):
            total = total + sums[sbs[s] * groups + grps[g]]
    wide = jnp.broadcast_to(total, (TILE, LANES))
    weight_sq = jnp.sum(jnp.where(lane_iota == sub_iota, wide, 0.0), axis=1, keepdims=True)
    update_sq = jnp.sum(jnp.where(lane_iota == sub_iota + LAYERS, wide, 0.0), axis=1, keepdims=True)
    ratio = learn_rate * (jnp.sqrt(weight_sq) / (jnp.sqrt(update_sq) + trust_eps))
    ratio_out[...] = jnp.broadcast_to(ratio, (TILE, LANES))

    for h in reversed(held_back):

        @pl.when(peer_holds(h))
        def _(h=h):
            exchange(h, across_all).wait_recv()
            consume(h, across_all, count=False)
            lend(h).wait_send()

    pltpu.make_async_remote_copy(
        src_ref=staged.at[pl.ds(1, devices - 1)],
        dst_ref=landed.at[pl.ds(1, devices - 1)],
        send_sem=send_sem,
        recv_sem=sum_recv,
        device_id=at(1, 0),
        device_id_type=MESH,
    ).wait_send()
    told.wait_send()


def finish(ratio_ref, row_ids, weights, update, first, second,
           fresh_hbm, first_hbm, second_hbm, fresh, fresh_sem, moment_sem):
    rows_dev, width = weights.shape
    columns = width // LANES
    moments = [
        pltpu.make_async_copy(first, first_hbm, moment_sem.at[0]),
        pltpu.make_async_copy(second, second_hbm, moment_sem.at[1]),
    ]
    for move in moments:
        move.start()
    ratio = ratio_ref[...]
    span = rows_dev // PIECES
    moves = []
    for p in range(PIECES):

        def step_rows(s, carry):
            base = pl.multiple_of(p * span + s * TILE, TILE)
            here = row_ids[pl.ds(base, TILE), :]
            step = jnp.zeros((TILE, LANES), jnp.float32)
            for t in range(LAYERS):
                step = jnp.where(here == t, jnp.broadcast_to(ratio[t : t + 1], (TILE, LANES)), step)
            for c in range(columns):
                cut = slice(c * LANES, (c + 1) * LANES)
                rows = pl.ds(base, TILE)
                fresh[rows, cut] = weights[rows, cut] - step * update[rows, cut]
            return carry

        lax.fori_loop(0, span // TILE, step_rows, 0)
        rows = pl.ds(p * span, span)
        moves.append(pltpu.make_async_copy(fresh.at[rows], fresh_hbm.at[rows], fresh_sem.at[p]))
        if p:
            moves[p - 1].start()
    moves[-1].start()
    for move in moves + moments:
        move.wait()


def local(groups, subs, master, moment_one, moment_two, gradient, partner, tensor_of_row):
    rows_dev, width = master.shape
    devices = groups * subs
    block = rows_dev // devices
    whole = jax.ShapeDtypeStruct((rows_dev, width), jnp.float32)
    vmem = pl.BlockSpec(memory_space=pltpu.VMEM)
    hbm = pl.BlockSpec(memory_space=pltpu.HBM)
    slots = (devices, 3, block, width)
    held_back = max(HELD)
    weights, update, first, second, row_ids, ratio = pl.pallas_call(
        functools.partial(kernel, groups, subs),
        out_shape=(
            *[pltpu.VMEM((rows_dev, width), jnp.float32)] * 4,
            pltpu.VMEM((rows_dev, LANES), jnp.int32),
            pltpu.VMEM((LAYERS, LANES), jnp.float32),
        ),
        in_specs=[hbm] * 6,
        out_specs=(vmem,) * 6,
        scratch_shapes=[
            pltpu.SMEM(partner.shape, jnp.int32),
            pltpu.SMEM(tensor_of_row.shape, jnp.int32),
        ]
        + [pltpu.VMEM((rows_dev // TILE, TILE, width), jnp.float32)] * 3
        + [
            pltpu.VMEM((rows_dev, width), jnp.float32),
            pltpu.VMEM(slots, jnp.float32),
            pltpu.VMEM(slots, jnp.float32),
            pltpu.VMEM((LAYERS, TILE, LANES), jnp.float32),
            pltpu.VMEM((LAYERS, TILE, LANES), jnp.float32),
            pltpu.VMEM((devices, 1, LANES), jnp.float32),
            pltpu.VMEM((held_back, TILE, width), jnp.float32),
            pltpu.VMEM((held_back, block, width), jnp.float32),
            pltpu.VMEM((held_back, block, width), jnp.float32),
        ]
        + [pltpu.SemaphoreType.REGULAR((diameter(groups, subs) - 1,))]
        + [pltpu.SemaphoreType.DMA] * 7
        + [pltpu.SemaphoreType.DMA((held_back,))] * 2
        + [pltpu.SemaphoreType.DMA((3,)), pltpu.SemaphoreType.DMA((subs + groups,))],
        compiler_params=pltpu.CompilerParams(
            collective_id=0, has_side_effects=True, vmem_limit_bytes=48 * 1024 * 1024
        ),
    )(*(
        pltpu.with_memory_space_constraint(x, pltpu.HBM)
        for x in (
            partner,
            tensor_of_row,
            *(x.reshape(rows_dev // TILE, TILE, width) for x in (master, moment_one, moment_two)),
            gradient,
        )
    ))
    return pl.pallas_call(
        finish,
        out_shape=(whole, whole, whole),
        in_specs=[vmem] * 6,
        out_specs=(hbm, hbm, hbm),
        scratch_shapes=[
            pltpu.VMEM((rows_dev, width), jnp.float32),
            pltpu.SemaphoreType.DMA((PIECES,)),
            pltpu.SemaphoreType.DMA((2,)),
        ],
        compiler_params=pltpu.CompilerParams(vmem_limit_bytes=32 * 1024 * 1024),
    )(ratio, row_ids, weights, update, first, second)


def solution(mesh):
    rows = P(("grp", "sub"), None)
    return jax.shard_map(
        functools.partial(local, mesh.shape["grp"], mesh.shape["sub"]),
        mesh=mesh,
        in_specs=(rows, rows, rows, rows, P(), P()),
        out_specs=(rows, rows, rows),
        check_vma=False,
    )
```

```python
import functools

import jax
import jax.numpy as jnp
from jax import lax
from jax.experimental import pallas as pl
from jax.experimental.pallas import tpu as pltpu
from jax.sharding import PartitionSpec as P

LAYERS = 8
LANES = 128
TILE = 8
PIECES = 4
HELD = (2, 2)
AHEAD = (2, 2)
MESH = pl.DeviceIdType.MESH

beta_one = 0.9
beta_two = 0.999
step_count = 10
adam_eps = 1e-06
trust_eps = 1e-06
learn_rate = 0.05
decay_rate = 0.01


def xor(a, b, bound):
    total, bit = 0, 1
    while bit < bound:
        total = total + ((a // bit + b // bit) % 2) * bit
        bit *= 2
    return total


def flips(here, bound):
    steps, bit = [], 1
    while bit < bound:
        steps.append(bit - 2 * bit * ((here // bit) % 2))
        bit *= 2
    return [
        here + sum(step for b, step in enumerate(steps) if (k >> b) % 2) for k in range(bound)
    ]


def sub_order(subs):
    width = subs.bit_length() - 1
    codes = [i ^ (i >> 1) for i in range(subs)]
    return [sum(((c >> b) & 1) << (width - 1 - b) for b in range(width)) for c in codes]


def near_links(groups, subs):
    bits = [1 << b for b in range(subs.bit_length() - 1)]
    flat = [(1 << b, 0) for b in range(groups.bit_length() - 1)]
    flat += [(0, bit) for bit in (bits if subs != 4 else bits[:1])]
    return flat, [(g, subs - 1) for g in range(2) if (g, subs - 1) not in flat]


def diameter(groups, subs):
    return groups.bit_length() - 1 + (3 if subs == 4 else subs.bit_length() - 1)


def kernel(groups, subs, partner_hbm, ids_hbm, master_hbm, one_hbm, two_hbm, grad_hbm,
           weights, update, first_out, second_out, row_ids, ratio_out,
           partner, ids, master, one, two, grad, staged, landed, acc_w, acc_u, sums,
           near, lent, borrowed, rounds, near_sem, partner_sem, ids_sem, grad_sem, send_sem,
           sum_send, sum_recv, lend_send, lend_recv, load_sem, recv_sem):
    devices = groups * subs
    rows_dev, width = grad.shape
    block = rows_dev // devices
    many = TILE // block
    columns = width // LANES
    my_grp, my_sub = lax.axis_index("grp"), lax.axis_index("sub")
    me = my_grp * subs + my_sub
    grps, sbs = flips(my_grp, groups), flips(my_sub, subs)
    order = sub_order(subs)
    send_order = order[1:] + order[:1]
    take_order = [s for s in order if s != subs - 1] + [subs - 1]
    peers = [(g, s) for s in send_order for g in range(groups) if g or s]
    across_all = subs - 1
    inner = (my_sub == subs // 2 - 1) | (my_sub == subs // 2)
    held_back = range(near.shape[0])
    odd = my_grp % 2

    def by_core(pair, core):
        return pair[0] + (pair[1] - pair[0]) * core

    def i_hold(g):
        return inner & (g < by_core(HELD, odd))

    def peer_holds(g):
        return inner & (g < by_core(HELD, (odd + g) % 2))

    def send_held(before):
        ahead = by_core(AHEAD, odd)
        for h in reversed(held_back):
            for a in range(3):
                turn = (by_core(HELD, odd) - 1 - h) * 3 + a
                now = turn < ahead if before else turn >= ahead
                pl.when(i_hold(h) & now)(exchange_array(h, across_all, a).start)

    def tile_of(place):
        return pl.ds(pl.multiple_of(place // many * TILE, TILE), TILE)

    def device_of(g, s):
        return grps[g] * subs + sbs[s]

    for h in held_back:
        pltpu.make_async_copy(
            grad_hbm.at[tile_of(device_of(h, across_all))], near.at[h], near_sem
        ).start()
    pltpu.make_async_copy(partner_hbm, partner, partner_sem).start()

    def at(g, s):
        return {"grp": grps[g], "sub": sbs[s]}

    flat, steep = near_links(groups, subs)

    def greet(sem):
        for g, s in flat:
            pl.semaphore_signal(sem, inc=1, device_id=at(g, s), device_id_type=MESH)

        @pl.when(inner)
        def _():
            for g, s in steep:
                pl.semaphore_signal(sem, inc=1, device_id=at(g, s), device_id_type=MESH)

    def hear(sem):
        @pl.when(inner)
        def _():
            pl.semaphore_wait(sem, len(flat) + len(steep))

        @pl.when(jnp.logical_not(inner))
        def _():
            pl.semaphore_wait(sem, len(flat))

    barrier = pltpu.get_barrier_semaphore()
    greet(barrier)

    def across(g, s):
        return {"grp": xor(my_grp, g, groups), "sub": xor(my_sub, s, subs)}

    def exchange(g, s):
        k = s * groups + g
        return pltpu.make_async_remote_copy(
            src_ref=staged.at[k],
            dst_ref=landed.at[k],
            send_sem=send_sem,
            recv_sem=arrival(g, s),
            device_id=across(g, s),
            device_id_type=MESH,
        )

    def exchange_array(g, s, a):
        k = s * groups + g
        return pltpu.make_async_remote_copy(
            src_ref=staged.at[k, a],
            dst_ref=landed.at[k, a],
            send_sem=send_sem,
            recv_sem=arrival(g, s),
            device_id=across(g, s),
            device_id_type=MESH,
        )

    def arrival(g, s):
        return recv_sem.at[subs + g] if s == across_all else recv_sem.at[s]

    def batch(s, count):
        run = pl.ds(s * groups + groups - count, count)
        return pltpu.make_async_remote_copy(
            src_ref=staged.at[run],
            dst_ref=landed.at[run],
            send_sem=send_sem,
            recv_sem=recv_sem.at[s % subs],
            device_id=at(1, 0),
            device_id_type=MESH,
        )

    def exchange_sum(g, s):
        return pltpu.make_async_remote_copy(
            src_ref=sums.at[0],
            dst_ref=sums.at[s * groups + g],
            send_sem=sum_send,
            recv_sem=sum_recv,
            device_id=at(g, s),
            device_id_type=MESH,
        )

    def rank_of(device):
        def seek(n, found):
            return jnp.where(partner[n] == device, n, found)

        return lax.fori_loop(0, devices, seek, jnp.int32(0), unroll=8)

    def lend(h):
        return pltpu.make_async_remote_copy(
            src_ref=lent.at[h],
            dst_ref=borrowed.at[h],
            send_sem=lend_send.at[h],
            recv_sem=lend_recv.at[h],
            device_id=at(h, across_all),
            device_id_type=MESH,
        )

    def cuts():
        return [slice(c * LANES, (c + 1) * LANES) for c in range(columns)]

    def pick(tile, part):
        piece = tile[:block]
        for i in range(1, many):
            piece = jnp.where(part == i, tile[i * block : (i + 1) * block], piece)
        return piece

    pltpu.make_async_copy(near, near, near_sem).wait()
    loads = [
        pltpu.make_async_copy(src, dst, sem)
        for src, dst, sem in [
            (master_hbm, master, load_sem.at[0]), (one_hbm, one, load_sem.at[1]),
            (two_hbm, two, load_sem.at[2]), (ids_hbm, ids, ids_sem), (grad_hbm, grad, grad_sem),
        ]
    ]
    for load in loads[:3]:
        load.start()
    for h in held_back:
        for cut in cuts():
            lent[h, :, cut] = pick(near[h, :, cut], device_of(h, across_all) % many)
    pltpu.make_async_copy(partner_hbm, partner, partner_sem).wait()

    def stage(g, s, target):
        there = across(g, s)
        rank = rank_of(there["grp"] * subs + there["sub"])
        slab, part = rank // many, jnp.full((block, LANES), rank % many, jnp.int32)
        for a, source in enumerate((master, one, two)):
            for cut in cuts():
                target[a, :, cut] = pick(source[slab, :, cut], part)

    hear(barrier)
    for h in held_back:
        pl.when(peer_holds(h))(lend(h).start)

    last_round = rounds.shape[0] - 1

    def next_round(r):
        hear(rounds.at[r])
        if r < last_round:
            greet(rounds.at[r + 1])

    greet(rounds.at[0])
    next_round(0)
    for load in loads[:3]:
        load.wait()
    for load in loads[3:]:
        load.start()
    for g in range(2):
        stage(g, send_order[0], staged.at[send_order[0] * groups + g])
    exchange(0, send_order[0]).start()
    next_round(1)
    exchange(1, send_order[0]).start()
    for r in range(2, last_round + 1):
        next_round(r)
    for s in send_order:
        begin = 2 if s == send_order[0] else 0 if s else 1
        if begin == groups:
            continue

        def step(i, s=s, begin=begin):
            if s == send_order[0]:
                return 2 + (groups - 3 - i + odd * 4) % (groups - 2)
            return xor(groups - 1 - i, odd * (groups // 2), groups) if s else groups - 1 - i

        def send_one(g, s=s):
            if s == across_all:
                pl.when(jnp.logical_not(i_hold(g)))(exchange(g, s).start)
            else:
                exchange(g, s).start()

        first_g = step(0)
        stage(first_g, s, staged.at[s * groups + first_g])

        def send(i, carry, s=s, step=step, send_one=send_one):
            g, later = step(i), step(i + 1)
            stage(later, s, staged.at[s * groups + later])
            send_one(g)
            return carry

        lax.fori_loop(0, groups - 1 - begin, send, 0)
        send_one(step(groups - 1 - begin))

    send_held(True)

    stage(0, 0, landed.at[0])
    my_rank = rank_of(me)
    for load in loads[3:]:
        load.wait()
    acc_w[...] = jnp.zeros_like(acc_w)
    acc_u[...] = jnp.zeros_like(acc_u)
    sub_iota = lax.broadcasted_iota(jnp.int32, (TILE, LANES), 0)
    lane_iota = lax.broadcasted_iota(jnp.int32, (TILE, LANES), 1)
    scale_one = 1.0 / (1.0 - beta_one**step_count)
    scale_two = 1.0 / (1.0 - beta_two**step_count)

    def moments(w, one, two, grown):
        first = beta_one * one + (1.0 - beta_one) * grown
        second = beta_two * two + (1.0 - beta_two) * grown * grown
        u = (first * scale_one) / (jnp.sqrt(second * scale_two) + adam_eps) + decay_rate * w
        return first, second, u

    def name_rows(start, part):
        here = jnp.full((TILE, LANES), -1, jnp.int32)
        for b in range(block):
            here = jnp.where(sub_iota == part * block + b, ids[start + b], here)
        return here

    def account(here, sum_w, sum_u):
        for t in range(LAYERS):
            acc_w[t] += jnp.where(here == t, sum_w, 0.0)
            acc_u[t] += jnp.where(here == t, sum_u, 0.0)

    def consume(g, s, count=True):
        there, k = across(g, s), s * groups + g
        source = there["grp"] * subs + there["sub"]
        rows, part = tile_of(source), source % many
        held = sub_iota // block == part
        here = name_rows(source * rows_dev + my_rank * block, part)
        row_ids[rows, :] = jnp.where(held, here, row_ids[rows, :])
        sum_w = jnp.zeros((TILE, LANES), jnp.float32)
        sum_u = jnp.zeros((TILE, LANES), jnp.float32)
        for cut in cuts():

            def arrived(a):
                return jnp.concatenate([landed[k, a, :, cut]] * many, axis=0)

            def put(ref, value):
                ref[rows, cut] = jnp.where(held, value, ref[rows, cut])

            w = arrived(0)
            first, second, u = moments(w, arrived(1), arrived(2), grad[rows, cut])
            put(first_out, first)
            put(second_out, second)
            put(weights, w)
            put(update, u)
            sum_w += w * w
            sum_u += u * u
        if count:
            account(here, sum_w, sum_u)

    def count_held(h):
        k = across_all * groups + h
        start = me * rows_dev + rank_of(device_of(h, across_all)) * block
        sum_w = jnp.zeros((block, LANES), jnp.float32)
        sum_u = jnp.zeros((block, LANES), jnp.float32)
        for cut in cuts():
            w = staged[k, 0, :, cut]
            _, _, u = moments(w, staged[k, 1, :, cut], staged[k, 2, :, cut], borrowed[h, :, cut])
            sum_w += w * w
            sum_u += u * u
        account(
            name_rows(start, 0),
            jnp.concatenate([sum_w] * many, axis=0),
            jnp.concatenate([sum_u] * many, axis=0),
        )

    consume(0, 0)
    for s in take_order:
        if s == across_all:

            for h in held_back:

                @pl.when(i_hold(h))
                def _(h=h):
                    lend(h).wait_recv()
                    count_held(h)

        else:
            batch(s, groups if s else groups - 1).wait_recv()

        def receive(i, carry, s=s):
            g = groups - 1 - i

            def take():
                exchange(g, s).wait_recv()
                consume(g, s)

            if s == across_all:
                pl.when(jnp.logical_not(peer_holds(g)))(take)
            else:
                consume(g, s)
            return carry

        lax.fori_loop(0, groups if s else groups - 1, receive, 0)

    col_w = jnp.sum(jnp.sum(acc_w[...], axis=1), axis=1, keepdims=True)
    col_u = jnp.sum(jnp.sum(acc_u[...], axis=1), axis=1, keepdims=True)
    spread = jnp.where(lane_iota == sub_iota, col_w, 0.0) + jnp.where(
        lane_iota == sub_iota + LAYERS, col_u, 0.0
    )
    sums[0] = jnp.sum(spread, axis=0, keepdims=True)
    for g, s in peers:
        exchange_sum(g, s).start()

    send_held(False)

    told = pltpu.make_async_remote_copy(
        src_ref=sums.at[pl.ds(1, devices - 1)],
        dst_ref=sums.at[pl.ds(1, devices - 1)],
        send_sem=sum_send,
        recv_sem=sum_recv,
        device_id=at(1, 0),
        device_id_type=MESH,
    )
    told.wait_recv()
    total = jnp.zeros((1, LANES), jnp.float32)
    for g in range(groups):
        for s in range(subs):
            total = total + sums[sbs[s] * groups + grps[g]]
    wide = jnp.broadcast_to(total, (TILE, LANES))
    weight_sq = jnp.sum(jnp.where(lane_iota == sub_iota, wide, 0.0), axis=1, keepdims=True)
    update_sq = jnp.sum(jnp.where(lane_iota == sub_iota + LAYERS, wide, 0.0), axis=1, keepdims=True)
    ratio = learn_rate * (jnp.sqrt(weight_sq) / (jnp.sqrt(update_sq) + trust_eps))
    ratio_out[...] = jnp.broadcast_to(ratio, (TILE, LANES))

    for h in reversed(held_back):

        @pl.when(peer_holds(h))
        def _(h=h):
            exchange(h, across_all).wait_recv()
            consume(h, across_all, count=False)
            lend(h).wait_send()

    pltpu.make_async_remote_copy(
        src_ref=staged.at[pl.ds(1, devices - 1)],
        dst_ref=landed.at[pl.ds(1, devices - 1)],
        send_sem=send_sem,
        recv_sem=sum_recv,
        device_id=at(1, 0),
        device_id_type=MESH,
    ).wait_send()
    told.wait_send()


def finish(ratio_ref, row_ids, weights, update, first, second,
           fresh_hbm, first_hbm, second_hbm, fresh, fresh_sem, moment_sem):
    rows_dev, width = weights.shape
    columns = width // LANES
    moments = [
        pltpu.make_async_copy(first, first_hbm, moment_sem.at[0]),
        pltpu.make_async_copy(second, second_hbm, moment_sem.at[1]),
    ]
    for move in moments:
        move.start()
    ratio = ratio_ref[...]
    span = rows_dev // PIECES
    moves = []
    for p in range(PIECES):

        def step_rows(s, carry):
            base = pl.multiple_of(p * span + s * TILE, TILE)
            here = row_ids[pl.ds(base, TILE), :]
            step = jnp.zeros((TILE, LANES), jnp.float32)
            for t in range(LAYERS):
                step = jnp.where(here == t, jnp.broadcast_to(ratio[t : t + 1], (TILE, LANES)), step)
            for c in range(columns):
                cut = slice(c * LANES, (c + 1) * LANES)
                rows = pl.ds(base, TILE)
                fresh[rows, cut] = weights[rows, cut] - step * update[rows, cut]
            return carry

        lax.fori_loop(0, span // TILE, step_rows, 0)
        rows = pl.ds(p * span, span)
        moves.append(pltpu.make_async_copy(fresh.at[rows], fresh_hbm.at[rows], fresh_sem.at[p]))
        if p:
            moves[p - 1].start()
    moves[-1].start()
    for move in moves + moments:
        move.wait()


def local(groups, subs, master, moment_one, moment_two, gradient, partner, tensor_of_row):
    rows_dev, width = master.shape
    devices = groups * subs
    block = rows_dev // devices
    whole = jax.ShapeDtypeStruct((rows_dev, width), jnp.float32)
    vmem = pl.BlockSpec(memory_space=pltpu.VMEM)
    hbm = pl.BlockSpec(memory_space=pltpu.HBM)
    slots = (devices, 3, block, width)
    held_back = max(HELD)
    weights, update, first, second, row_ids, ratio = pl.pallas_call(
        functools.partial(kernel, groups, subs),
        out_shape=(
            *[pltpu.VMEM((rows_dev, width), jnp.float32)] * 4,
            pltpu.VMEM((rows_dev, LANES), jnp.int32),
            pltpu.VMEM((LAYERS, LANES), jnp.float32),
        ),
        in_specs=[hbm] * 6,
        out_specs=(vmem,) * 6,
        scratch_shapes=[
            pltpu.SMEM(partner.shape, jnp.int32),
            pltpu.SMEM(tensor_of_row.shape, jnp.int32),
        ]
        + [pltpu.VMEM((rows_dev // TILE, TILE, width), jnp.float32)] * 3
        + [
            pltpu.VMEM((rows_dev, width), jnp.float32),
            pltpu.VMEM(slots, jnp.float32),
            pltpu.VMEM(slots, jnp.float32),
            pltpu.VMEM((LAYERS, TILE, LANES), jnp.float32),
            pltpu.VMEM((LAYERS, TILE, LANES), jnp.float32),
            pltpu.VMEM((devices, 1, LANES), jnp.float32),
            pltpu.VMEM((held_back, TILE, width), jnp.float32),
            pltpu.VMEM((held_back, block, width), jnp.float32),
            pltpu.VMEM((held_back, block, width), jnp.float32),
        ]
        + [pltpu.SemaphoreType.REGULAR((diameter(groups, subs) - 1,))]
        + [pltpu.SemaphoreType.DMA] * 7
        + [pltpu.SemaphoreType.DMA((held_back,))] * 2
        + [pltpu.SemaphoreType.DMA((3,)), pltpu.SemaphoreType.DMA((subs + groups,))],
        compiler_params=pltpu.CompilerParams(
            collective_id=0, has_side_effects=True, vmem_limit_bytes=48 * 1024 * 1024
        ),
    )(*(
        pltpu.with_memory_space_constraint(x, pltpu.HBM)
        for x in (
            partner,
            tensor_of_row,
            *(x.reshape(rows_dev // TILE, TILE, width) for x in (master, moment_one, moment_two)),
            gradient,
        )
    ))
    return pl.pallas_call(
        finish,
        out_shape=(whole, whole, whole),
        in_specs=[vmem] * 6,
        out_specs=(hbm, hbm, hbm),
        scratch_shapes=[
            pltpu.VMEM((rows_dev, width), jnp.float32),
            pltpu.SemaphoreType.DMA((PIECES,)),
            pltpu.SemaphoreType.DMA((2,)),
        ],
        compiler_params=pltpu.CompilerParams(vmem_limit_bytes=32 * 1024 * 1024),
    )(ratio, row_ids, weights, update, first, second)


def solution(mesh):
    rows = P(("grp", "sub"), None)
    return jax.shard_map(
        functools.partial(local, mesh.shape["grp"], mesh.shape["sub"]),
        mesh=mesh,
        in_specs=(rows, rows, rows, rows, P(), P()),
        out_specs=(rows, rows, rows),
        check_vma=False,
    )
```

```python
import functools

import jax
import jax.numpy as jnp
from jax import lax
from jax.experimental import pallas as pl
from jax.experimental.pallas import tpu as pltpu
from jax.sharding import PartitionSpec as P

LAYERS = 8
LANES = 128
TILE = 8
PIECES = 4
HELD = (2, 2)
AHEAD = (2, 3)
MESH = pl.DeviceIdType.MESH

beta_one = 0.9
beta_two = 0.999
step_count = 10
adam_eps = 1e-06
trust_eps = 1e-06
learn_rate = 0.05
decay_rate = 0.01


def xor(a, b, bound):
    total, bit = 0, 1
    while bit < bound:
        total = total + ((a // bit + b // bit) % 2) * bit
        bit *= 2
    return total


def flips(here, bound):
    steps, bit = [], 1
    while bit < bound:
        steps.append(bit - 2 * bit * ((here // bit) % 2))
        bit *= 2
    return [
        here + sum(step for b, step in enumerate(steps) if (k >> b) % 2) for k in range(bound)
    ]


def sub_order(subs):
    width = subs.bit_length() - 1
    codes = [i ^ (i >> 1) for i in range(subs)]
    return [sum(((c >> b) & 1) << (width - 1 - b) for b in range(width)) for c in codes]


def near_links(groups, subs):
    bits = [1 << b for b in range(subs.bit_length() - 1)]
    flat = [(1 << b, 0) for b in range(groups.bit_length() - 1)]
    flat += [(0, bit) for bit in (bits if subs != 4 else bits[:1])]
    return flat, [(g, subs - 1) for g in range(2) if (g, subs - 1) not in flat]


def diameter(groups, subs):
    return groups.bit_length() - 1 + (3 if subs == 4 else subs.bit_length() - 1)


def kernel(groups, subs, partner_hbm, ids_hbm, master_hbm, one_hbm, two_hbm, grad_hbm,
           weights, update, first_out, second_out, row_ids, ratio_out,
           partner, ids, master, one, two, grad, staged, landed, acc_w, acc_u, sums,
           near, lent, borrowed, rounds, near_sem, partner_sem, ids_sem, grad_sem, send_sem,
           sum_send, sum_recv, lend_send, lend_recv, load_sem, recv_sem):
    devices = groups * subs
    rows_dev, width = grad.shape
    block = rows_dev // devices
    many = TILE // block
    columns = width // LANES
    my_grp, my_sub = lax.axis_index("grp"), lax.axis_index("sub")
    me = my_grp * subs + my_sub
    grps, sbs = flips(my_grp, groups), flips(my_sub, subs)
    order = sub_order(subs)
    send_order = order[1:] + order[:1]
    take_order = [s for s in order if s != subs - 1] + [subs - 1]
    peers = [(g, s) for s in send_order for g in range(groups) if g or s]
    across_all = subs - 1
    inner = (my_sub == subs // 2 - 1) | (my_sub == subs // 2)
    held_back = range(near.shape[0])
    odd = my_grp % 2

    def by_core(pair, core):
        return pair[0] + (pair[1] - pair[0]) * core

    def i_hold(g):
        return inner & (g < by_core(HELD, odd))

    def peer_holds(g):
        return inner & (g < by_core(HELD, (odd + g) % 2))

    def send_held(before):
        ahead = by_core(AHEAD, odd)
        for h in reversed(held_back):
            for a in range(3):
                turn = (by_core(HELD, odd) - 1 - h) * 3 + a
                now = turn < ahead if before else turn >= ahead
                pl.when(i_hold(h) & now)(exchange_array(h, across_all, a).start)

    def tile_of(place):
        return pl.ds(pl.multiple_of(place // many * TILE, TILE), TILE)

    def device_of(g, s):
        return grps[g] * subs + sbs[s]

    for h in held_back:
        pltpu.make_async_copy(
            grad_hbm.at[tile_of(device_of(h, across_all))], near.at[h], near_sem
        ).start()
    pltpu.make_async_copy(partner_hbm, partner, partner_sem).start()

    def at(g, s):
        return {"grp": grps[g], "sub": sbs[s]}

    flat, steep = near_links(groups, subs)

    def greet(sem):
        for g, s in flat:
            pl.semaphore_signal(sem, inc=1, device_id=at(g, s), device_id_type=MESH)

        @pl.when(inner)
        def _():
            for g, s in steep:
                pl.semaphore_signal(sem, inc=1, device_id=at(g, s), device_id_type=MESH)

    def hear(sem):
        @pl.when(inner)
        def _():
            pl.semaphore_wait(sem, len(flat) + len(steep))

        @pl.when(jnp.logical_not(inner))
        def _():
            pl.semaphore_wait(sem, len(flat))

    barrier = pltpu.get_barrier_semaphore()
    greet(barrier)

    def across(g, s):
        return {"grp": xor(my_grp, g, groups), "sub": xor(my_sub, s, subs)}

    def exchange(g, s):
        k = s * groups + g
        return pltpu.make_async_remote_copy(
            src_ref=staged.at[k],
            dst_ref=landed.at[k],
            send_sem=send_sem,
            recv_sem=arrival(g, s),
            device_id=across(g, s),
            device_id_type=MESH,
        )

    def exchange_array(g, s, a):
        k = s * groups + g
        return pltpu.make_async_remote_copy(
            src_ref=staged.at[k, a],
            dst_ref=landed.at[k, a],
            send_sem=send_sem,
            recv_sem=arrival(g, s),
            device_id=across(g, s),
            device_id_type=MESH,
        )

    def arrival(g, s):
        return recv_sem.at[subs + g] if s == across_all else recv_sem.at[s]

    def batch(s, count):
        run = pl.ds(s * groups + groups - count, count)
        return pltpu.make_async_remote_copy(
            src_ref=staged.at[run],
            dst_ref=landed.at[run],
            send_sem=send_sem,
            recv_sem=recv_sem.at[s % subs],
            device_id=at(1, 0),
            device_id_type=MESH,
        )

    def exchange_sum(g, s):
        return pltpu.make_async_remote_copy(
            src_ref=sums.at[0],
            dst_ref=sums.at[s * groups + g],
            send_sem=sum_send,
            recv_sem=sum_recv,
            device_id=at(g, s),
            device_id_type=MESH,
        )

    def rank_of(device):
        def seek(n, found):
            return jnp.where(partner[n] == device, n, found)

        return lax.fori_loop(0, devices, seek, jnp.int32(0), unroll=8)

    def lend(h):
        return pltpu.make_async_remote_copy(
            src_ref=lent.at[h],
            dst_ref=borrowed.at[h],
            send_sem=lend_send.at[h],
            recv_sem=lend_recv.at[h],
            device_id=at(h, across_all),
            device_id_type=MESH,
        )

    def cuts():
        return [slice(c * LANES, (c + 1) * LANES) for c in range(columns)]

    def pick(tile, part):
        piece = tile[:block]
        for i in range(1, many):
            piece = jnp.where(part == i, tile[i * block : (i + 1) * block], piece)
        return piece

    pltpu.make_async_copy(near, near, near_sem).wait()
    loads = [
        pltpu.make_async_copy(src, dst, sem)
        for src, dst, sem in [
            (master_hbm, master, load_sem.at[0]), (one_hbm, one, load_sem.at[1]),
            (two_hbm, two, load_sem.at[2]), (ids_hbm, ids, ids_sem), (grad_hbm, grad, grad_sem),
        ]
    ]
    for load in loads[:3]:
        load.start()
    for h in held_back:
        for cut in cuts():
            lent[h, :, cut] = pick(near[h, :, cut], device_of(h, across_all) % many)
    pltpu.make_async_copy(partner_hbm, partner, partner_sem).wait()

    def stage(g, s, target):
        there = across(g, s)
        rank = rank_of(there["grp"] * subs + there["sub"])
        slab, part = rank // many, jnp.full((block, LANES), rank % many, jnp.int32)
        for a, source in enumerate((master, one, two)):
            for cut in cuts():
                target[a, :, cut] = pick(source[slab, :, cut], part)

    hear(barrier)
    for h in held_back:
        pl.when(peer_holds(h))(lend(h).start)

    last_round = rounds.shape[0] - 1

    def next_round(r):
        hear(rounds.at[r])
        if r < last_round:
            greet(rounds.at[r + 1])

    greet(rounds.at[0])
    next_round(0)
    for load in loads[:3]:
        load.wait()
    for load in loads[3:]:
        load.start()
    for g in range(2):
        stage(g, send_order[0], staged.at[send_order[0] * groups + g])
    exchange(0, send_order[0]).start()
    next_round(1)
    exchange(1, send_order[0]).start()
    for r in range(2, last_round + 1):
        next_round(r)
    for s in send_order:
        begin = 2 if s == send_order[0] else 0 if s else 1
        if begin == groups:
            continue

        def step(i, s=s, begin=begin):
            if s == send_order[0]:
                return 2 + (groups - 3 - i + odd * 4) % (groups - 2)
            return xor(groups - 1 - i, odd * (groups // 4), groups) if s else groups - 1 - i

        def send_one(g, s=s):
            if s == across_all:
                pl.when(jnp.logical_not(i_hold(g)))(exchange(g, s).start)
            else:
                exchange(g, s).start()

        first_g = step(0)
        stage(first_g, s, staged.at[s * groups + first_g])

        def send(i, carry, s=s, step=step, send_one=send_one):
            g, later = step(i), step(i + 1)
            stage(later, s, staged.at[s * groups + later])
            send_one(g)
            return carry

        lax.fori_loop(0, groups - 1 - begin, send, 0)
        send_one(step(groups - 1 - begin))

    send_held(True)

    stage(0, 0, landed.at[0])
    my_rank = rank_of(me)
    for load in loads[3:]:
        load.wait()
    acc_w[...] = jnp.zeros_like(acc_w)
    acc_u[...] = jnp.zeros_like(acc_u)
    sub_iota = lax.broadcasted_iota(jnp.int32, (TILE, LANES), 0)
    lane_iota = lax.broadcasted_iota(jnp.int32, (TILE, LANES), 1)
    scale_one = 1.0 / (1.0 - beta_one**step_count)
    scale_two = 1.0 / (1.0 - beta_two**step_count)

    def moments(w, one, two, grown):
        first = beta_one * one + (1.0 - beta_one) * grown
        second = beta_two * two + (1.0 - beta_two) * grown * grown
        u = (first * scale_one) / (jnp.sqrt(second * scale_two) + adam_eps) + decay_rate * w
        return first, second, u

    def name_rows(start, part):
        here = jnp.full((TILE, LANES), -1, jnp.int32)
        for b in range(block):
            here = jnp.where(sub_iota == part * block + b, ids[start + b], here)
        return here

    def account(here, sum_w, sum_u):
        for t in range(LAYERS):
            acc_w[t] += jnp.where(here == t, sum_w, 0.0)
            acc_u[t] += jnp.where(here == t, sum_u, 0.0)

    def consume(g, s, count=True):
        there, k = across(g, s), s * groups + g
        source = there["grp"] * subs + there["sub"]
        rows, part = tile_of(source), source % many
        held = sub_iota // block == part
        here = name_rows(source * rows_dev + my_rank * block, part)
        row_ids[rows, :] = jnp.where(held, here, row_ids[rows, :])
        sum_w = jnp.zeros((TILE, LANES), jnp.float32)
        sum_u = jnp.zeros((TILE, LANES), jnp.float32)
        for cut in cuts():

            def arrived(a):
                return jnp.concatenate([landed[k, a, :, cut]] * many, axis=0)

            def put(ref, value):
                ref[rows, cut] = jnp.where(held, value, ref[rows, cut])

            w = arrived(0)
            first, second, u = moments(w, arrived(1), arrived(2), grad[rows, cut])
            put(first_out, first)
            put(second_out, second)
            put(weights, w)
            put(update, u)
            sum_w += w * w
            sum_u += u * u
        if count:
            account(here, sum_w, sum_u)

    def count_held(h):
        k = across_all * groups + h
        start = me * rows_dev + rank_of(device_of(h, across_all)) * block
        sum_w = jnp.zeros((block, LANES), jnp.float32)
        sum_u = jnp.zeros((block, LANES), jnp.float32)
        for cut in cuts():
            w = staged[k, 0, :, cut]
            _, _, u = moments(w, staged[k, 1, :, cut], staged[k, 2, :, cut], borrowed[h, :, cut])
            sum_w += w * w
            sum_u += u * u
        account(
            name_rows(start, 0),
            jnp.concatenate([sum_w] * many, axis=0),
            jnp.concatenate([sum_u] * many, axis=0),
        )

    consume(0, 0)
    for s in take_order:
        if s == across_all:

            for h in held_back:

                @pl.when(i_hold(h))
                def _(h=h):
                    lend(h).wait_recv()
                    count_held(h)

        else:
            batch(s, groups if s else groups - 1).wait_recv()

        def receive(i, carry, s=s):
            g = groups - 1 - i

            def take():
                exchange(g, s).wait_recv()
                consume(g, s)

            if s == across_all:
                pl.when(jnp.logical_not(peer_holds(g)))(take)
            else:
                consume(g, s)
            return carry

        lax.fori_loop(0, groups if s else groups - 1, receive, 0)

    col_w = jnp.sum(jnp.sum(acc_w[...], axis=1), axis=1, keepdims=True)
    col_u = jnp.sum(jnp.sum(acc_u[...], axis=1), axis=1, keepdims=True)
    spread = jnp.where(lane_iota == sub_iota, col_w, 0.0) + jnp.where(
        lane_iota == sub_iota + LAYERS, col_u, 0.0
    )
    sums[0] = jnp.sum(spread, axis=0, keepdims=True)
    for g, s in peers:
        exchange_sum(g, s).start()

    send_held(False)

    told = pltpu.make_async_remote_copy(
        src_ref=sums.at[pl.ds(1, devices - 1)],
        dst_ref=sums.at[pl.ds(1, devices - 1)],
        send_sem=sum_send,
        recv_sem=sum_recv,
        device_id=at(1, 0),
        device_id_type=MESH,
    )
    told.wait_recv()
    total = jnp.zeros((1, LANES), jnp.float32)
    for g in range(groups):
        for s in range(subs):
            total = total + sums[sbs[s] * groups + grps[g]]
    wide = jnp.broadcast_to(total, (TILE, LANES))
    weight_sq = jnp.sum(jnp.where(lane_iota == sub_iota, wide, 0.0), axis=1, keepdims=True)
    update_sq = jnp.sum(jnp.where(lane_iota == sub_iota + LAYERS, wide, 0.0), axis=1, keepdims=True)
    ratio = learn_rate * (jnp.sqrt(weight_sq) / (jnp.sqrt(update_sq) + trust_eps))
    ratio_out[...] = jnp.broadcast_to(ratio, (TILE, LANES))

    for h in reversed(held_back):

        @pl.when(peer_holds(h))
        def _(h=h):
            exchange(h, across_all).wait_recv()
            consume(h, across_all, count=False)
            lend(h).wait_send()

    pltpu.make_async_remote_copy(
        src_ref=staged.at[pl.ds(1, devices - 1)],
        dst_ref=landed.at[pl.ds(1, devices - 1)],
        send_sem=send_sem,
        recv_sem=sum_recv,
        device_id=at(1, 0),
        device_id_type=MESH,
    ).wait_send()
    told.wait_send()


def finish(ratio_ref, row_ids, weights, update, first, second,
           fresh_hbm, first_hbm, second_hbm, fresh, fresh_sem, moment_sem):
    rows_dev, width = weights.shape
    columns = width // LANES
    moments = [
        pltpu.make_async_copy(first, first_hbm, moment_sem.at[0]),
        pltpu.make_async_copy(second, second_hbm, moment_sem.at[1]),
    ]
    for move in moments:
        move.start()
    ratio = ratio_ref[...]
    span = rows_dev // PIECES
    moves = []
    for p in range(PIECES):

        def step_rows(s, carry):
            base = pl.multiple_of(p * span + s * TILE, TILE)
            here = row_ids[pl.ds(base, TILE), :]
            step = jnp.zeros((TILE, LANES), jnp.float32)
            for t in range(LAYERS):
                step = jnp.where(here == t, jnp.broadcast_to(ratio[t : t + 1], (TILE, LANES)), step)
            for c in range(columns):
                cut = slice(c * LANES, (c + 1) * LANES)
                rows = pl.ds(base, TILE)
                fresh[rows, cut] = weights[rows, cut] - step * update[rows, cut]
            return carry

        lax.fori_loop(0, span // TILE, step_rows, 0)
        rows = pl.ds(p * span, span)
        moves.append(pltpu.make_async_copy(fresh.at[rows], fresh_hbm.at[rows], fresh_sem.at[p]))
        if p:
            moves[p - 1].start()
    moves[-1].start()
    for move in moves + moments:
        move.wait()


def local(groups, subs, master, moment_one, moment_two, gradient, partner, tensor_of_row):
    rows_dev, width = master.shape
    devices = groups * subs
    block = rows_dev // devices
    whole = jax.ShapeDtypeStruct((rows_dev, width), jnp.float32)
    vmem = pl.BlockSpec(memory_space=pltpu.VMEM)
    hbm = pl.BlockSpec(memory_space=pltpu.HBM)
    slots = (devices, 3, block, width)
    held_back = max(HELD)
    weights, update, first, second, row_ids, ratio = pl.pallas_call(
        functools.partial(kernel, groups, subs),
        out_shape=(
            *[pltpu.VMEM((rows_dev, width), jnp.float32)] * 4,
            pltpu.VMEM((rows_dev, LANES), jnp.int32),
            pltpu.VMEM((LAYERS, LANES), jnp.float32),
        ),
        in_specs=[hbm] * 6,
        out_specs=(vmem,) * 6,
        scratch_shapes=[
            pltpu.SMEM(partner.shape, jnp.int32),
            pltpu.SMEM(tensor_of_row.shape, jnp.int32),
        ]
        + [pltpu.VMEM((rows_dev // TILE, TILE, width), jnp.float32)] * 3
        + [
            pltpu.VMEM((rows_dev, width), jnp.float32),
            pltpu.VMEM(slots, jnp.float32),
            pltpu.VMEM(slots, jnp.float32),
            pltpu.VMEM((LAYERS, TILE, LANES), jnp.float32),
            pltpu.VMEM((LAYERS, TILE, LANES), jnp.float32),
            pltpu.VMEM((devices, 1, LANES), jnp.float32),
            pltpu.VMEM((held_back, TILE, width), jnp.float32),
            pltpu.VMEM((held_back, block, width), jnp.float32),
            pltpu.VMEM((held_back, block, width), jnp.float32),
        ]
        + [pltpu.SemaphoreType.REGULAR((diameter(groups, subs) - 1,))]
        + [pltpu.SemaphoreType.DMA] * 7
        + [pltpu.SemaphoreType.DMA((held_back,))] * 2
        + [pltpu.SemaphoreType.DMA((3,)), pltpu.SemaphoreType.DMA((subs + groups,))],
        compiler_params=pltpu.CompilerParams(
            collective_id=0, has_side_effects=True, vmem_limit_bytes=48 * 1024 * 1024
        ),
    )(*(
        pltpu.with_memory_space_constraint(x, pltpu.HBM)
        for x in (
            partner,
            tensor_of_row,
            *(x.reshape(rows_dev // TILE, TILE, width) for x in (master, moment_one, moment_two)),
            gradient,
        )
    ))
    return pl.pallas_call(
        finish,
        out_shape=(whole, whole, whole),
        in_specs=[vmem] * 6,
        out_specs=(hbm, hbm, hbm),
        scratch_shapes=[
            pltpu.VMEM((rows_dev, width), jnp.float32),
            pltpu.SemaphoreType.DMA((PIECES,)),
            pltpu.SemaphoreType.DMA((2,)),
        ],
        compiler_params=pltpu.CompilerParams(vmem_limit_bytes=32 * 1024 * 1024),
    )(ratio, row_ids, weights, update, first, second)


def solution(mesh):
    rows = P(("grp", "sub"), None)
    return jax.shard_map(
        functools.partial(local, mesh.shape["grp"], mesh.shape["sub"]),
        mesh=mesh,
        in_specs=(rows, rows, rows, rows, P(), P()),
        out_specs=(rows, rows, rows),
        check_vma=False,
    )
```
